32 devices in a mesh: seq: 8 (over z, y), feat: 4 (over x, core).
Axes of the slice: x: 2, y: 2, z: 4, core: 2. Of those that a mesh axis runs over, the one named last changes fastest.
Arguments:
- hidden_in: bfloat16 [4, 2048, 2048], P(None, 'seq'), may hold values from -6 to 6
- w_query: bfloat16 [2048, 256], replicated, may hold values from -0.125 to 0.125
- w_key: bfloat16 [2048, 256], replicated, may hold values from -0.125 to 0.125
- w_value: bfloat16 [2048, 2048], P(None, 'feat'), may hold values from -0.125 to 0.125
- lengths: int32 [4], replicated, may hold values from 1024 to 2048, as said below
- owners: int32 [4], replicated, may hold values from 0 to 7
Outputs:
- mixed: bfloat16 [4, 2048, 2048], P(None, 'seq', 'feat')
- state_quad: float32 [8, 4, 16, 256, 128], P('seq', None, None, 'feat')
- state_low: float32 [8, 4, 16, 17, 128], P('seq', None, 'feat')
- norm_quad: float32 [8, 4, 16, 256], P('seq', None, None, 'feat')
- norm_low: float32 [8, 4, 16, 17], P('seq', None, 'feat')
The draws below stay inside these ranges and needn't reach their ends.
Inputs may be any that keep to these rules, and one draw needn't show every extreme that they name: `lengths`: every prompt holds 1024 to 2048 live tokens, and some prompt holds exactly 2048. `owners`: several prompts may share a decoding device.
All inputs are finite; a program needn't handle non-finite values.
Results may differ from the reference program's by a relative error of at most 0.0085.
Values may be sent and summed in bfloat16 or wider, within the bound.
A program may use at most 256 MiB of HBM per device.

```python
import jax
import jax.numpy as jnp
from jax import lax

D = 2048
H = 16
HD = 128
FD = 16
PROMPTS = 4
SPAN = 256
LENGTH = 2048
N_SEQ = 8


def draw_lengths(key, part):
    first_key, second_key = jax.random.split(jax.random.fold_in(key, 11))
    drawn = jax.random.randint(first_key, (PROMPTS,), LENGTH // 2, LENGTH + 1)
    longest = jax.random.randint(second_key, (), 0, PROMPTS)
    return jnp.where(jnp.arange(PROMPTS) == longest, LENGTH, drawn).astype(jnp.int32)


def touch_ends(array, stream_key, least, top_value):
    dims = array.shape
    spot = [jax.random.randint(jax.random.fold_in(stream_key, axis), (), 0, dims[axis]) for axis in range(len(dims))]
    array = array.at[tuple(spot)].set(least)
    longest = dims.index(max(dims))
    spot[longest] = (spot[longest] + 1) % dims[longest]
    return array.at[tuple(spot)].set(top_value)


def levels(stream_key, shape, shards, low, largest):
    def one(axis_at, parts):
        draws = jax.random.uniform(jax.random.fold_in(jax.random.fold_in(stream_key, 6), axis_at), (parts,), jnp.float32, low / len(shards), largest / len(shards))
        return jnp.repeat(jnp.exp(draws), shape[axis_at] // parts).reshape((-1,) + (1,) * (len(shape) - axis_at - 1))

    level = one(*shards[0])
    for cut in shards[1:]:
        level = level * one(*cut)
    return level


def noise(own_key, shape, spread, most, cuts=(), held_as=jnp.bfloat16):
    array = jax.random.normal(own_key, shape, jnp.float32) * spread
    if len(cuts) > 0:
        array = levels(own_key, shape, cuts, -0.22, 0.18) * array
    return jnp.clip(array, min=-most, max=most).astype(held_as)


def setup_inputs(seed: int = 0) -> dict:
    streams_of = jax.random.split(jax.random.key(seed), 7)
    hidden_in = noise(streams_of[0], (PROMPTS, LENGTH, D), 1.0, 6.0, ((1, 8),))
    w_query = noise(streams_of[1], (D, H * FD), D ** -0.5, 0.125)
    w_key = noise(streams_of[2], (D, H * FD), D ** -0.5, 0.125)
    w_value = noise(streams_of[3], (D, D), D ** -0.5, 0.125, ((1, 4),))
    lengths = draw_lengths(jax.random.fold_in(streams_of[6], 71), 0)
    owners = touch_ends(jax.random.randint(streams_of[5], (PROMPTS,), 0, N_SEQ), jax.random.fold_in(streams_of[5], 1), 0, N_SEQ - 1).astype(jnp.int32)
    return dict(hidden_in=hidden_in, w_query=w_query, w_key=w_key, w_value=w_value, lengths=lengths, owners=owners)


NORM_FLOOR = 0.0001

def low_features(inputs):
    constant = jnp.ones(inputs.shape[:-1] + (1,), jnp.float32)
    return jnp.concatenate([constant, inputs * FD ** (-0.25)], axis=-1)

def quad_features(leading, inputs):
    products = leading[..., :, None] * inputs[..., None, :]
    return products.reshape(inputs.shape[:-1] + (leading.shape[-1] * inputs.shape[-1],)) * (2.0 * FD) ** (-0.5)

def reference(hidden_in, w_query, w_key, w_value, lengths, owners):
    highest = lax.Precision.HIGHEST
    n_blocks = LENGTH // SPAN

    def per_prompt(prompt_item):
        tokens, length = prompt_item
        queries = jnp.dot(tokens, w_query, preferred_element_type=jnp.float32).astype(jnp.bfloat16)
        key_rows = jnp.dot(tokens, w_key, preferred_element_type=jnp.float32).astype(jnp.bfloat16)
        values = jnp.dot(tokens, w_value, preferred_element_type=jnp.float32).astype(jnp.bfloat16)
        query_blocks = queries.astype(jnp.float32).reshape(n_blocks, SPAN, H, FD)
        key_blocks = key_rows.astype(jnp.float32).reshape(n_blocks, SPAN, H, FD)
        value_blocks = values.astype(jnp.float32).reshape(n_blocks, SPAN, H, HD)
        starts = jnp.arange(n_blocks, dtype=jnp.int32) * SPAN
        causal = (jnp.arange(SPAN)[:, None] >= jnp.arange(SPAN)[None, :]).astype(jnp.float32)

        def advance(carried, block_data):
            state_lo, state_qu, norm_lo, norm_qu = carried
            query_blk, key_blk, value_blk, start = block_data
            positions = start + jnp.arange(SPAN, dtype=jnp.int32)
            live_mask = (positions < length).astype(jnp.float32)
            query_low = low_features(query_blk)
            query_quad = quad_features(query_blk, query_blk)
            key_low = low_features(key_blk) * live_mask[:, None, None]
            key_quad = quad_features(key_blk, key_blk) * live_mask[:, None, None]
            numerator = jnp.einsum('thf,hfd->thd', query_low, state_lo, precision=highest)
            numerator = numerator + jnp.einsum('thf,hfd->thd', query_quad, state_qu, precision=highest)
            denominator = jnp.einsum('thf,hf->th', query_low, norm_lo, precision=highest)
            denominator = denominator + jnp.einsum('thf,hf->th', query_quad, norm_qu, precision=highest)
            scores = jnp.einsum('thf,uhf->htu', query_blk, key_blk, precision=highest)
            kernel = 1.0 + scores * FD ** (-0.5) + scores * scores * (0.5 / FD)
            weight = kernel * causal[None, :, :] * live_mask[None, None, :]
            numerator = numerator + jnp.einsum('htu,uhd->thd', weight, value_blk, precision=highest)
            denominator = denominator + lax.optimization_barrier(jnp.sum(weight, axis=2)).T
            attended = numerator / denominator[:, :, None] * live_mask[:, None, None]
            new_carried = (state_lo + jnp.einsum('thf,thd->hfd', key_low, value_blk, precision=highest), state_qu + jnp.einsum('thf,thd->hfd', key_quad, value_blk, precision=highest), norm_lo + lax.optimization_barrier(jnp.sum(key_low, axis=0)), norm_qu + lax.optimization_barrier(jnp.sum(key_quad, axis=0)))
            return (new_carried, attended.reshape(SPAN, H * HD))
        initial = (jnp.zeros((H, FD + 1, HD), jnp.float32), jnp.zeros((H, FD * FD, HD), jnp.float32), jnp.zeros((H, FD + 1), jnp.float32), jnp.zeros((H, FD * FD), jnp.float32))
        finals, attended = lax.scan(advance, initial, (query_blocks, key_blocks, value_blocks, starts))
        attended = attended.reshape(LENGTH, H * HD)
        mean_square = lax.optimization_barrier(jnp.mean(attended * attended, axis=-1))
        mixed = (attended * lax.rsqrt(mean_square + NORM_FLOOR)[:, None]).astype(jnp.bfloat16)
        return (mixed, finals)
    mixed, finals = lax.map(per_prompt, (hidden_in, lengths))
    final_low, final_quad, final_lnorm, final_qnorm = finals
    owner_table = (jnp.arange(N_SEQ, dtype=jnp.int32)[:, None] == owners[None, :]).astype(jnp.float32)
    state_quad = owner_table[:, :, None, None, None] * final_quad[None]
    state_low = owner_table[:, :, None, None, None] * final_low[None]
    norm_quad = owner_table[:, :, None, None] * final_qnorm[None]
    norm_low = owner_table[:, :, None, None] * final_lnorm[None]
    return (mixed, state_quad, state_low, norm_quad, norm_low)
```

```python
import functools

import jax
import jax.numpy as jnp
from jax import lax
from jax.experimental import pallas as pl
from jax.experimental.pallas import tpu as pltpu
from jax.sharding import PartitionSpec as P

H = 16
FD = 16
NORM_FLOOR = 0.0001
LANES = 128
BF = jnp.bfloat16
F32 = jnp.float32
LIN = 128
FAR = 144
ONE = 152
LIVE_ROWS = 153

NN = (((1,), (0,)), ((), ()))
NT = (((1,), (1,)), ((), ()))
TN = (((0,), (0,)), ((), ()))


def dot(a, b, dims=NN, precision=None):
    return lax.dot_general(a, b, dims, preferred_element_type=F32, precision=precision)


def iota(shape, axis):
    return lax.broadcasted_iota(jnp.int32, shape, axis)


def features(t, rows, weights):
    diag, off, lin = weights
    tokens = t.shape[1]
    blocks = [t * t * diag if diag != 1.0 else t * t]
    scaled = t * off if off != 1.0 else t
    for o in range(1, FD // 2):
        blocks.append(scaled * pltpu.roll(t, FD - o, 0))
    blocks.append(t * lin if lin != 1.0 else t)
    blocks.append(scaled[: FD // 2] * t[FD // 2 :])
    blocks.append((iota((rows - ONE, tokens), 0) == 0).astype(F32))
    return jnp.concatenate(blocks, axis=0)


def pick_matrix(first_row, count, rows):
    r = iota((count, rows), 0) + first_row
    c = iota((count, rows), 1)
    i, j = r >> 4, r & 15
    o = (j - i) & 15
    place = jnp.where(
        o < 8, o * FD + i, jnp.where(o == 8, FAR + jnp.minimum(i, j), (FD - o) * FD + j)
    )
    return (place == c)


def kernel(cfg, len_ref, x_hbm, wq_hbm, wk_hbm, wv_hbm,
           att_out, sqgot, quad_out, low_out, ztgot,
           hid, wqk, wv, qs, ks, vs, nd, part, mgot, bsend, got, presend, prer, fwd, pre, tot,
           tsend, sqsend, ztsend,
           in_sem, s0, r0, s1, r1, s2, r2, s3, r3, s4, r4, s5, r5, s6, r6, s7, r7, s8, r8):
    n, nf, npr, span, heads, rows, sub = cfg
    me, fi = lax.axis_index("seq"), lax.axis_index("feat")
    own = heads * FD
    outer_n = n // 2
    zo, yi = me // 2, lax.rem(me, 2)
    mate = me + 1 - 2 * yi
    zpeer = 2 * lax.rem(zo + 1, outer_n) + yi
    head_dim = vs.shape[2] // heads

    base = pl.multiple_of((fi * own // LANES) * LANES, LANES)
    loads = [
        pltpu.make_async_copy(wq_hbm.at[:, pl.ds(base, LANES)], wqk.at[:, pl.ds(0, LANES)], in_sem.at[npr]),
        pltpu.make_async_copy(wk_hbm.at[:, pl.ds(base, LANES)], wqk.at[:, pl.ds(LANES, LANES)], in_sem.at[npr + 1]),
        pltpu.make_async_copy(wv_hbm, wv, in_sem.at[npr + 2]),
    ]
    last = outer_n - 1

    def hid_copy(p):
        return pltpu.make_async_copy(x_hbm.at[p], hid.at[p], in_sem.at[p])

    loads[0].start()
    loads[1].start()
    hid_copy(0).start()
    loads[2].start()
    for step in range(1, npr):
        hid_copy(step).start()

    barrier = pltpu.get_barrier_semaphore()

    @pl.loop(1, n)
    def _(i):
        pl.semaphore_signal(barrier, 1, device_id={"seq": lax.rem(me + i, n)}, device_id_type=pl.DeviceIdType.MESH)

    for i in range(1, nf):
        pl.semaphore_signal(barrier, 1, device_id={"feat": lax.rem(fi + i, nf)}, device_id_type=pl.DeviceIdType.MESH)

    def to_seq(src, dst, ssem, rsem, target):
        return pltpu.make_async_remote_copy(
            src_ref=src, dst_ref=dst, send_sem=ssem, recv_sem=rsem,
            device_id={"seq": target}, device_id_type=pl.DeviceIdType.MESH)

    def to_feat(src, dst, ssem, rsem, target):
        return pltpu.make_async_remote_copy(
            src_ref=src, dst_ref=dst, send_sem=ssem, recv_sem=rsem,
            device_id={"feat": target}, device_id_type=pl.DeviceIdType.MESH)

    peer = lax.rem(me + 1, n)
    fpeer = lax.rem(fi + 1, nf)
    for load in loads:
        load.wait()

    def live_row(p):
        return ((iota((1, span), 1) + me * span) < len_ref[p]).astype(F32)

    def own_half(block):
        out = block[:, :own]
        for r in range(1, LANES // own):
            out = jnp.where(lax.rem(fi, LANES // own) == r, block[:, r * own:(r + 1) * own], out)
        return out

    def project(p, _):
        hid_copy(p).wait()
        x = hid[p]
        qk = dot(x, wqk[...])
        q = own_half(qk[:, :LANES]).astype(BF)
        k = own_half(qk[:, LANES:]).astype(BF)
        qs[p] = q
        ks[p] = k
        v = dot(x, wv[...]).astype(BF)
        vs[p] = v
        kt = k.astype(F32).T
        live = live_row(p)
        sums = []
        tail = rows - ONE
        row = iota((tail, LANES), 0)
        ones = jnp.ones((tail, span), BF)
        gap = jnp.zeros((tail, 2 * LANES - ONE - 8), F32)
        for h in range(heads):
            phi = (features(kt[h * FD:(h + 1) * FD], rows, (1.0, 1.0, 1.0)) * live).astype(BF)
            summed = dot(phi, v[:, h * head_dim:(h + 1) * head_dim])
            zh = dot(ones, phi, NT)
            more = jnp.concatenate([zh[:, LANES:ONE + 8], gap], axis=1)
            end = summed[ONE:] + jnp.where(row == 1, zh[:, :LANES], 0.0) + jnp.where(row == 2, more, 0.0)
            sums.append(jnp.concatenate([summed[:ONE], end], axis=0).astype(BF))
        half = heads // 2
        for c in range(2):
            part[p, c] = jnp.concatenate(sums[c * half:(c + 1) * half], axis=0).reshape(outer_n, sub, head_dim)

        @pl.when(p == 0)
        def _():
            pl.semaphore_wait(barrier, n - 1 + nf - 1)
        to_seq(part.at[p, 1 - yi], mgot.at[p], s0.at[p], r0.at[p], mate).start()

        @pl.when(p > 0)
        def _():
            pair_up(p - 1)
        return 0

    def pair_up(p):
        to_seq(bsend.at[p], mgot.at[p], s0.at[p], r0.at[p], mate).wait_recv()
        bsend[p] = (part[p, yi].astype(F32) + mgot[p].astype(F32)).astype(BF)
        got[p, zo] = bsend[p, zo]

        @pl.loop(1, outer_n)
        def _(i):
            there = lax.rem(zo + i, outer_n)
            to_seq(bsend.at[p, there], got.at[p, zo], s1.at[p, i], r1.at[p, zo], 2 * there + yi).start()

    def home(p):
        def scan(z, acc):
            @pl.when(z != zo)
            def _():
                to_seq(bsend.at[p, z], got.at[p, z], s1.at[p, z], r1.at[p, z], zpeer).wait_recv()
            presend[p, z] = acc.astype(BF)
            return acc + got[p, z].astype(F32)

        total = lax.fori_loop(0, outer_n, scan, jnp.zeros((sub, head_dim), F32))
        tot[p, yi, zo] = total.astype(BF)
        prer[p, zo] = presend[p, zo]

        @pl.loop(1, outer_n)
        def _(i):
            there = lax.rem(zo + i, outer_n)

            @pl.when(there != 0)
            def _():
                to_seq(presend.at[p, there], prer.at[p, zo], s2.at[p, i], r2.at[p, zo], 2 * there + yi).start()

        @pl.loop(1, outer_n)
        def _(i):
            there = lax.rem(zo + i, outer_n)

            @pl.when(there != last)
            def _():
                to_seq(tot.at[p, yi, zo], tot.at[p, yi, zo], s3.at[p, i], r3.at[p, zo], 2 * there + yi).start()

    def take_prefix(p):
        @pl.when(zo != 0)
        def _():
            @pl.loop(1, outer_n)
            def _(i):
                there = lax.rem(zo + i, outer_n)
                to_seq(presend.at[p, there], prer.at[p, there], s2.at[p, i], r2.at[p, there], zpeer).wait_recv()

        @pl.when(zo == 0)
        def _():
            prer[p] = jnp.zeros(prer.shape[1:], BF)
        before = prer[p].astype(F32)
        fwd[p] = (before + jnp.where(yi == 0, part[p, yi].astype(F32), 0.0)).astype(BF)
        to_seq(fwd.at[p], pre.at[p, yi], s7.at[p], r7.at[p], mate).start()
        pre[p, yi] = (before + jnp.where(yi == 1, mgot[p].astype(F32), 0.0)).astype(BF)

    def take_total(p):
        @pl.when(zo != last)
        def _():
            @pl.loop(1, outer_n)
            def _(i):
                there = lax.rem(zo + i, outer_n)
                to_seq(presend.at[p, there], tot.at[p, yi, there], s3.at[p, i], r3.at[p, there], zpeer).wait_recv()
            to_seq(tot.at[p, yi], tot.at[p, yi], s8.at[p], r8.at[p], mate).start()

        @pl.when(zo == last)
        def _():
            @pl.loop(1, outer_n)
            def _(i):
                there = lax.rem(zo + i, outer_n)
                tot[p, yi, there] = (prer[p, there].astype(F32) + bsend[p, there].astype(F32)).astype(BF)
            to_seq(tot.at[p, yi], tot.at[p, yi], s8.at[p], r8.at[p], mate).start()

    lax.fori_loop(0, npr, project, 0)

    def inner(p, _):
        causal = iota((span, span), 0) >= iota((span, span), 1)
        keep = jnp.where(causal, live_row(p), 0.0)
        ones = jnp.ones((span, head_dim), BF)
        for h in range(heads):
            s = dot(qs[p, :, h * FD:(h + 1) * FD], ks[p, :, h * FD:(h + 1) * FD], NT)
            w = ((1.0 + s * (FD ** -0.5 + s * (0.5 / FD))) * keep).astype(BF)
            vv = jnp.concatenate([vs[p, :, h * head_dim:(h + 1) * head_dim], ones], axis=1)
            nd[p, h] = dot(w, vv)
        return 0

    sqsend[...] = jnp.zeros_like(sqsend)
    weights = (0.5 / FD, 1.0 / FD, FD ** -0.5)

    def joined(ref, p):
        return jnp.concatenate([ref[p, c].reshape(outer_n * sub, head_dim) for c in range(2)], axis=0)

    def zrow_of(state, h):
        block = state[h * rows + LIN:h * rows + ONE + 8].astype(F32)
        return jnp.concatenate([block[ONE + 1 - LIN:ONE + 2 - LIN], block[ONE + 2 - LIN:ONE + 3 - LIN, :ONE + 8 - LANES]], axis=1)

    def outer(p):
        to_seq(fwd.at[p], pre.at[p, 1 - yi], s7.at[p], r7.at[p], mate).wait_recv()
        qt = qs[p].astype(F32).T
        state = joined(pre, p)
        live = (iota((span, 1), 0) + me * span < len_ref[p]).astype(F32)
        earlier = jnp.minimum(me * span, len_ref[p]).astype(F32)
        sq = jnp.zeros((sqsend.shape[0], span), F32)
        for h in range(heads):
            phi = features(qt[h * FD:(h + 1) * FD], rows, weights).astype(BF)
            zr = zrow_of(state, h)
            zr = jnp.where(iota(zr.shape, 1) == ONE, 0.0, zr)
            zb = jnp.broadcast_to(zr, (head_dim, zr.shape[1])).astype(BF)
            phit = phi.T
            num = dot(phit, state[h * rows:(h + 1) * rows]) + nd[p, h, :, :head_dim]
            den = dot(phit[:, :zr.shape[1]], zb, NT) + nd[p, h, :, head_dim:] + earlier
            att = num / den * live
            att_out[p, :, h * head_dim:(h + 1) * head_dim] = att
            sq = sq + dot(jnp.ones((sqsend.shape[0], head_dim), BF), (att * att).astype(BF), NT)
        sqsend[...] = jnp.where(iota(sq.shape, 0) == p, sq, sqsend[...])

    ztsend[...] = jnp.zeros_like(ztsend)
    per = FD * FD // nf
    pick = pick_matrix(0, FD * FD, rows).astype(BF)

    def spread(p):
        to_seq(tot.at[p, yi], tot.at[p, 1 - yi], s8.at[p], r8.at[p], mate).wait_recv()
        state = joined(tot, p)
        zt = ztsend[...]
        zrow = iota(zt.shape, 0)
        for h in range(heads):
            mine = state[h * rows:(h + 1) * rows]
            zr = zrow_of(state, h)
            zr = jnp.where(iota(zr.shape, 1) == ONE, len_ref[p].astype(F32), zr)
            zt = jnp.where(zrow == p * heads + h, zr, zt)
            full = dot(pick, mine).astype(BF)
            for f in range(nf):
                tsend[f, p, h] = full[f * per:(f + 1) * per]
            tail = mine[LIN:].astype(F32)
            low_out[p, h] = jnp.concatenate(
                [tail[ONE - LIN:ONE - LIN + 1], tail[:FD] * FD ** -0.25], axis=0)
        ztsend[...] = zt
        for i in range(1, nf):
            target = lax.rem(fi + i, nf)
            to_feat(tsend.at[target, p], quad_out.at[fi, p], s5.at[i, p], r5.at[fi, p], target).start()

    lax.fori_loop(0, npr // 2, inner, 0)
    home(0)
    lax.fori_loop(npr // 2, npr, inner, 0)
    for p in range(1, npr - 2):
        home(p)
    for p in range(npr):
        if p == 0:
            pair_up(npr - 1)
        take_prefix(p)
        take_total(p)
        if p + npr - 2 < npr:
            home(p + npr - 2)
        if p > 0:
            outer(p - 1)
            spread(p - 1)
    outer(npr - 1)

    sqgot[fi] = sqsend[...]
    for i in range(1, nf):
        to_feat(sqsend, sqgot.at[fi], s4.at[i], r4.at[fi], lax.rem(fi + i, nf)).start()

    spread(npr - 1)
    zt = ztsend[...]
    ztgot[fi] = zt
    for i in range(1, nf):
        to_feat(ztsend, ztgot.at[fi], s6.at[i], r6.at[fi], lax.rem(fi + i, nf)).start()
    quad_out[fi] = tsend[fi]

    for i in range(1, nf):
        src = lax.rem(fi + i, nf)
        to_feat(sqsend, sqgot.at[src], s4.at[i], r4.at[src], fpeer).wait_recv()
    for i in range(1, nf):
        src = lax.rem(fi + i, nf)
        to_feat(ztsend, ztgot.at[src], s6.at[i], r6.at[src], fpeer).wait_recv()
    for i in range(1, nf):
        src = lax.rem(fi + i, nf)

        @pl.loop(0, npr)
        def _(p):
            to_feat(tsend.at[src, p], quad_out.at[src, p], s5.at[i, p], r5.at[src, p], fpeer).wait_recv()
            to_feat(tsend.at[src, p], quad_out.at[src, p], s5.at[i, p], r5.at[src, p], fpeer).wait_send()
        to_feat(sqsend, sqgot.at[fi], s4.at[i], r4.at[fi], fpeer).wait_send()
        to_feat(ztsend, ztgot.at[fi], s6.at[i], r6.at[fi], fpeer).wait_send()

    @pl.loop(0, npr)
    def _(p):
        to_seq(part.at[p, yi], mgot.at[p], s0.at[p], r0.at[p], mate).wait_send()
        to_seq(fwd.at[p], pre.at[p, yi], s7.at[p], r7.at[p], mate).wait_send()
        to_seq(tot.at[p, yi], tot.at[p, yi], s8.at[p], r8.at[p], mate).wait_send()

        @pl.loop(1, outer_n)
        def _(i):
            there = lax.rem(zo + i, outer_n)
            to_seq(bsend.at[p, there], got.at[p, zo], s1.at[p, i], r1.at[p, zo], zpeer).wait_send()

            @pl.when(there != 0)
            def _():
                to_seq(presend.at[p, there], prer.at[p, zo], s2.at[p, i], r2.at[p, zo], zpeer).wait_send()

            @pl.when(there != last)
            def _():
                to_seq(tot.at[p, yi, zo], tot.at[p, yi, zo], s3.at[p, i], r3.at[p, zo], zpeer).wait_send()


def finish(cfg, own_ref, att, sq, quad, low, zt, mixed_out, quad_out, low_out, nq_out, nl_out,
           mixed_buf, quad_buf, sem):
    nf, heads, npr, per = cfg
    span, width = att.shape[1], att.shape[2]
    fi, me = lax.axis_index("feat"), lax.axis_index("seq")
    squares = sq[0]
    for f in range(1, nf):
        squares = squares + sq[f]
    inv = lax.rsqrt(squares * (1.0 / (nf * width)) + NORM_FLOOR)
    writes = []
    for p in range(npr):
        mask = (own_ref[p] == me).astype(F32)
        for f in range(nf):
            quad_buf[p, f * heads:(f + 1) * heads] = quad[f, p].astype(F32) * (mask * (2.0 * FD) ** -0.5)
        writes.append(pltpu.make_async_copy(quad_buf.at[p], quad_out.at[p], sem.at[0, p]))
        writes[-1].start()
        col = jnp.broadcast_to(inv[p:p + 1], (LANES, span)).T
        for c in range(width // LANES):
            mixed_buf[p, :, c * LANES:(c + 1) * LANES] = (att[p, :, c * LANES:(c + 1) * LANES] * col).astype(BF)
        writes.append(pltpu.make_async_copy(mixed_buf.at[p], mixed_out.at[p], sem.at[1, p]))
        writes[-1].start()
    own_pick = pick_matrix(fi * per, per, ONE + 8).astype(F32)
    lr, lc = iota((FD + 1, ONE + 8), 0), iota((FD + 1, ONE + 8), 1)
    low_pick = jnp.where(lr == 0, (lc == ONE).astype(F32), (lc == LIN - 1 + lr).astype(F32) * FD ** -0.25)
    nl = dot(zt[fi], low_pick, NT, lax.Precision.HIGHEST)
    for f in range(nf):
        nq = dot(zt[f], own_pick, NT, lax.Precision.HIGHEST) * (2.0 * FD) ** -0.5
        for p in range(npr):
            mask = (own_ref[p] == me).astype(F32)
            nq_out[p, f * heads:(f + 1) * heads] = nq[p * heads:(p + 1) * heads] * mask
    for p in range(npr):
        mask = (own_ref[p] == me).astype(F32)
        nl_out[p] = nl[p * heads:(p + 1) * heads] * mask
        for h in range(heads):
            low_out[p, :, h, :] = low[p, h] * mask
    for write in writes:
        write.wait()


def body(hidden_in, w_query, w_key, w_value, lengths, owners):
    npr, span, width = hidden_in.shape
    n, nf = lax.axis_size("seq"), lax.axis_size("feat")
    heads = H // nf
    head_dim = width // H
    step = 16 * n // heads
    rows = -(-LIVE_ROWS // 8) * 8
    rows = -(-rows // step) * step
    sub = heads * rows // n
    cfg = (n, nf, npr, span, heads, rows, sub)
    per = FD * FD // nf
    dma = pltpu.SemaphoreType.DMA
    vm = pltpu.VMEM
    ph = npr * heads
    out = pl.pallas_call(
        functools.partial(kernel, cfg),
        out_shape=(
            vm((npr, span, heads * head_dim), F32),
            vm((nf, 8, span), F32),
            vm((nf, npr, heads, per, head_dim), BF),
            vm((npr, heads, FD + 1, head_dim), F32),
            vm((nf, ph, ONE + 8), F32),
        ),
        in_specs=[pl.BlockSpec(memory_space=pltpu.SMEM)] + [pl.BlockSpec(memory_space=pltpu.HBM)] * 4,
        out_specs=[pl.BlockSpec(memory_space=pltpu.VMEM)] * 5,
        scratch_shapes=[
            vm((npr, span, width), BF),
            vm((width, 2 * LANES), BF),
            vm((width, heads * head_dim), BF),
            vm((npr, span, heads * FD), BF),
            vm((npr, span, heads * FD), BF),
            vm((npr, span, heads * head_dim), BF),
            vm((npr, heads, span, 2 * head_dim), F32),
            vm((npr, 2, n // 2, sub, head_dim), BF),
            vm((npr, n // 2, sub, head_dim), BF),
            vm((npr, n // 2, sub, head_dim), BF),
            vm((npr, n // 2, sub, head_dim), BF),
            vm((npr, n // 2, sub, head_dim), BF),
            vm((npr, n // 2, sub, head_dim), BF),
            vm((npr, n // 2, sub, head_dim), BF),
            vm((npr, 2, n // 2, sub, head_dim), BF),
            vm((npr, 2, n // 2, sub, head_dim), BF),
            vm((nf, npr, heads, per, head_dim), BF),
            vm((8, span), F32),
            vm((ph, ONE + 8), F32),
            dma((npr + 3,)),
            dma((npr,)), dma((npr,)), dma((npr, n // 2)), dma((npr, n // 2)),
            dma((npr, n // 2)), dma((npr, n // 2)), dma((npr, n // 2)), dma((npr, n // 2)),
            dma((nf,)), dma((nf,)), dma((nf, npr)), dma((nf, npr)), dma((nf,)), dma((nf,)),
            dma((npr,)), dma((npr,)), dma((npr,)), dma((npr,)),
        ],
        compiler_params=pltpu.CompilerParams(
            collective_id=0, has_side_effects=True, vmem_limit_bytes=40 * 1024 * 1024
        ),
        name="layer",
    )(lengths, *[pltpu.with_memory_space_constraint(a, pltpu.HBM) for a in (hidden_in, w_query, w_key, w_value)])
    onchip = [pltpu.with_memory_space_constraint(o, pltpu.VMEM) for o in out]
    block = pl.BlockSpec
    mixed, quad, low, nq, nl = pl.pallas_call(
        functools.partial(finish, (nf, heads, npr, per)),
        out_shape=(
            jax.ShapeDtypeStruct((npr, span, heads * head_dim), BF),
            jax.ShapeDtypeStruct((npr, H, per, head_dim), F32),
            jax.ShapeDtypeStruct((npr, FD + 1, heads, head_dim), F32),
            jax.ShapeDtypeStruct((npr, H, per), F32),
            jax.ShapeDtypeStruct((npr, heads, FD + 1), F32),
        ),
        in_specs=[block(memory_space=pltpu.SMEM)] + [block(memory_space=pltpu.VMEM)] * 5,
        out_specs=[block(memory_space=pl.ANY)] * 2 + [block(memory_space=pltpu.VMEM)] * 3,
        scratch_shapes=[
            vm((npr, span, heads * head_dim), BF),
            vm((npr, H, per, head_dim), F32),
            dma((2, npr)),
        ],
        compiler_params=pltpu.CompilerParams(vmem_limit_bytes=16 * 1024 * 1024),
        name="finish",
    )(owners, *onchip)
    return (mixed, quad[None], jnp.transpose(low, (0, 2, 1, 3))[None], nq[None], nl[None])


def solution(mesh):
    placed = (P(None, "seq", None), P(), P(), P(None, "feat"), P(), P())
    return jax.shard_map(
        body,
        mesh=mesh,
        in_specs=placed,
        out_specs=(
            P(None, "seq", "feat"),
            P("seq", None, None, "feat", None),
            P("seq", None, "feat", None, None),
            P("seq", None, None, "feat"),
            P("seq", None, "feat", None),
        ),
        check_vma=False,
    )
```

```python
import functools

import jax
import jax.numpy as jnp
from jax import lax
from jax.experimental import pallas as pl
from jax.experimental.pallas import tpu as pltpu
from jax.sharding import PartitionSpec as P

H = 16
FD = 16
NORM_FLOOR = 0.0001
LANES = 128
BF = jnp.bfloat16
F32 = jnp.float32
LIN = 128
FAR = 144
ONE = 152
LIVE_ROWS = 153

NN = (((1,), (0,)), ((), ()))
NT = (((1,), (1,)), ((), ()))
TN = (((0,), (0,)), ((), ()))


def dot(a, b, dims=NN, precision=None):
    return lax.dot_general(a, b, dims, preferred_element_type=F32, precision=precision)


def iota(shape, axis):
    return lax.broadcasted_iota(jnp.int32, shape, axis)


def features(t, rows, weights):
    diag, off, lin = weights
    tokens = t.shape[1]
    blocks = [t * t * diag if diag != 1.0 else t * t]
    scaled = t * off if off != 1.0 else t
    for o in range(1, FD // 2):
        blocks.append(scaled * pltpu.roll(t, FD - o, 0))
    blocks.append(t * lin if lin != 1.0 else t)
    blocks.append(scaled[: FD // 2] * t[FD // 2 :])
    blocks.append((iota((rows - ONE, tokens), 0) == 0).astype(F32))
    return jnp.concatenate(blocks, axis=0)


def pick_matrix(first_row, count, rows):
    r = iota((count, rows), 0) + first_row
    c = iota((count, rows), 1)
    i, j = r >> 4, r & 15
    o = (j - i) & 15
    place = jnp.where(
        o < 8, o * FD + i, jnp.where(o == 8, FAR + jnp.minimum(i, j), (FD - o) * FD + j)
    )
    return (place == c)


def kernel(cfg, len_hbm, own_hbm, x_hbm, wq_hbm, wk_hbm, wv_hbm,
           att_out, sqgot, quad_out, low_out, ztgot, mine_out,
           hid, wall, qs, ks, vs, kt, phs, nd, part, mgot, bsum, up_got, up_send, dn_got, dn_send,
           fwd, pre, bwd, suf, tsend, sqsend, ztsend, len_ref, own_ref,
           in_sem, s0, r0, s1, r1, s2, r2, s3, r3, s4, r4, s5, r5, s6, r6, s7, r7):
    n, nf, npr, span, heads, rows, cpp, lag, turn = cfg
    me, fi = lax.axis_index("seq"), lax.axis_index("feat")
    own = heads * FD
    half = heads // 2
    last = n // 2 - 1
    zo, yi = me // 2, lax.rem(me, 2)
    mate = me + 1 - 2 * yi
    head_dim = vs.shape[2] // heads
    spot = lax.rem(fi * own, LANES)
    hw = half * head_dim
    chunks = npr * cpp
    below, above = zo > 0, zo < last

    def half_cols(c):
        return pl.ds(pl.multiple_of(c * hw, LANES), hw)

    base = pl.multiple_of((fi * own // LANES) * LANES, LANES)
    qk_loads = [
        pltpu.make_async_copy(wq_hbm.at[:, pl.ds(base, LANES)], wall.at[:, pl.ds(0, LANES)], in_sem.at[npr]),
        pltpu.make_async_copy(wk_hbm.at[:, pl.ds(base, LANES)], wall.at[:, pl.ds(LANES, LANES)], in_sem.at[npr + 1]),
    ]

    def v_load(step):
        cols = half_cols(1 - yi if step == 0 else yi)
        return pltpu.make_async_copy(wv_hbm.at[:, cols], wall.at[:, pl.ds(2 * LANES + step * hw, hw)], in_sem.at[npr + 2 + step])

    def hid_copy(p):
        return pltpu.make_async_copy(x_hbm.at[p], hid.at[p], in_sem.at[p])

    for load in qk_loads:
        load.start()
    hid_copy(0).start()
    v_load(0).start()
    v_load(1).start()
    small = [
        pltpu.make_async_copy(len_hbm, len_ref, in_sem.at[npr + 4]),
        pltpu.make_async_copy(own_hbm, own_ref, in_sem.at[npr + 5]),
    ]
    for load in small:
        load.start()

    barrier = pltpu.get_barrier_semaphore()

    def greet(axis, target):
        pl.semaphore_signal(barrier, 1, device_id={axis: target}, device_id_type=pl.DeviceIdType.MESH)

    greet("seq", mate)

    @pl.when(below)
    def _():
        greet("seq", me - 2)

    @pl.when(above)
    def _():
        greet("seq", me + 2)

    for i in range(1, nf):
        greet("feat", lax.rem(fi + i, nf))

    @pl.when(zo == 0)
    def _():
        up_got[...] = jnp.zeros(up_got.shape, BF)

    @pl.when(zo == last)
    def _():
        dn_got[...] = jnp.zeros(dn_got.shape, BF)

    def to_seq(src, dst, ssem, rsem, target):
        return pltpu.make_async_remote_copy(
            src_ref=src, dst_ref=dst, send_sem=ssem, recv_sem=rsem,
            device_id={"seq": target}, device_id_type=pl.DeviceIdType.MESH)

    def to_feat(src, dst, ssem, rsem, target):
        return pltpu.make_async_remote_copy(
            src_ref=src, dst_ref=dst, send_sem=ssem, recv_sem=rsem,
            device_id={"feat": target}, device_id_type=pl.DeviceIdType.MESH)

    fpeer = lax.rem(fi + 1, nf)

    def swap_copy(p, j):
        return to_seq(part.at[p, 0, j], mgot.at[p, j], s0, r0.at[p, j], mate)

    def up_copy(p, j):
        return to_seq(up_send.at[p, j], up_got.at[p, j], s1, r1.at[p, j], me + 2 * above.astype(jnp.int32) - 2 * (1 - above.astype(jnp.int32)))

    def dn_copy(p, j):
        return to_seq(dn_send.at[p, j], dn_got.at[p, j], s2, r2.at[p, j], me - 2 * below.astype(jnp.int32) + 2 * (1 - below.astype(jnp.int32)))

    def pre_copy(p, j):
        return to_seq(fwd.at[p, j], pre.at[p, 0, j], s3, r3.at[p, j], mate)

    def suf_copy(p, j):
        return to_seq(bwd.at[p, j], suf.at[p, j], s7, r7.at[p, j], mate)

    def live_row(p):
        return ((iota((1, span), 1) + me * span) < len_ref[p]).astype(F32)

    tail = rows - ONE
    weights = (0.5 / FD, 1.0 / FD, FD ** -0.5)

    def sums_of(slot, side, v, live):
        row = iota((tail, LANES), 0)
        ones = jnp.ones((tail, span), BF)
        gap = jnp.zeros((tail, 2 * LANES - ONE - 8), F32)
        sums = []
        for h in range(half):
            phi = (features(kt[side, head_rows(slot + h)], rows, (1.0, 1.0, 1.0)) * live).astype(BF)
            summed = dot(phi, v[:, h * head_dim:(h + 1) * head_dim])
            zh = dot(ones, phi, NT)
            more = jnp.concatenate([zh[:, LANES:ONE + 8], gap], axis=1)
            end = summed[ONE:] + jnp.where(row == 1, zh[:, :LANES], 0.0) + jnp.where(row == 2, more, 0.0)
            sums.append(jnp.concatenate([summed[:ONE], end], axis=0).astype(BF))
        return jnp.concatenate(sums, axis=0).reshape(part.shape[2:])

    def head_of(slot):
        return (1 - yi if slot < half else yi) * half + slot % half

    def head_rows(slot):
        return pl.ds(pl.multiple_of(spot + head_of(slot) * FD, FD), FD)

    for load in qk_loads:
        load.wait()
    v_load(0).wait()
    for load in small:
        load.wait()
    hid_copy(0).wait()
    for p in range(1, npr):
        hid_copy(p).start()
    middle = wall.shape[0] // 2

    def project(p, first):
        if not first:
            hid_copy(p).wait()
        x = hid[p]
        head = dot(x, wall[:, :2 * LANES + hw])
        k = head[:, LANES:2 * LANES].astype(BF)
        qs[p] = head[:, :LANES].astype(BF)
        ks[p] = k
        slot = lax.rem(p, 2)
        kt[slot] = k.astype(F32).T
        v = head[:, 2 * LANES:].astype(BF)
        vs[p, :, :hw] = v
        if first:
            v_load(1).wait()
        else:
            late(p - 1)
        mine = dot(x[:, :middle], wall[:middle, 2 * LANES + hw:]) + dot(x[:, middle:], wall[middle:, 2 * LANES + hw:])
        part[p, 0] = sums_of(0, slot, v, live_row(p))
        vs[p, :, hw:] = mine.astype(BF)
        if first:
            pl.semaphore_wait(barrier, nf + below.astype(jnp.int32) + above.astype(jnp.int32))
        for j in range(cpp):
            swap_copy(p, j).start()

    def late(p):
        part[p, 1] = sums_of(half, lax.rem(p, 2), vs[p, :, hw:], live_row(p))

    def pair(k):
        p, j = k // cpp, lax.rem(k, cpp)
        swap_copy(p, j).wait_recv()
        bsum[p, j] = (part[p, 1, j].astype(F32) + mgot[p, j].astype(F32)).astype(BF)

    def take_up(k):
        p, j = k // cpp, lax.rem(k, cpp)

        @pl.when(below)
        def _():
            up_copy(p, j).wait_recv()
        before = up_got[p, j].astype(F32)

        @pl.when(above)
        def _():
            up_send[p, j] = (up_got[p, j].astype(F32) + bsum[p, j].astype(F32)).astype(BF)
            up_copy(p, j).start()
        fwd[p, j] = (before + jnp.where(yi == 0, part[p, 1, j].astype(F32), 0.0)).astype(BF)
        pre_copy(p, j).start()
        pre[p, 1, j] = (before + jnp.where(yi == 1, mgot[p, j].astype(F32), 0.0)).astype(BF)

    def take_down(k):
        p, j = k // cpp, lax.rem(k, cpp)

        @pl.when(above)
        def _():
            dn_copy(p, j).wait_recv()
        after = dn_got[p, j].astype(F32)

        @pl.when(below)
        def _():
            dn_send[p, j] = (dn_got[p, j].astype(F32) + bsum[p, j].astype(F32)).astype(BF)
            dn_copy(p, j).start()
        bwd[p, j] = (after + jnp.where(yi == 1, part[p, 1, j].astype(F32), 0.0)).astype(BF)
        suf_copy(p, j).start()

    def at(t, body, stride=1):
        @pl.when((t >= 0) & (t < chunks) & (lax.rem(t, stride) == 0))
        def _():
            body(t // stride)

    def chain(t):
        at(t, pair)
        at(t - lag * zo, take_up)
        at(t - lag * (last - zo), take_down)

    project(0, True)

    @pl.loop(1, npr)
    def _(p):
        project(p, False)

        @pl.loop(jnp.maximum(p - 2, 0) * cpp, (p - 1) * cpp)
        def _(t):
            chain(t)

    late(npr - 1)
    for p in range(npr):
        mine_out[p] = jnp.broadcast_to((own_ref[p] == me).astype(F32), mine_out.shape[1:])

    def inner(p):
        causal = iota((span, span), 0) >= iota((span, span), 1)
        keep = jnp.where(causal, live_row(p), 0.0)
        ones = jnp.ones((span, head_dim), BF)
        lane = iota((1, LANES), 1) // FD
        q, k = qs[p], ks[p].astype(F32)
        kt[0] = q.astype(F32).T
        for h in range(heads):
            mask = (lane == spot // FD + head_of(h)).astype(F32)
            s = dot(q, (k * mask).astype(BF), NT)
            w = ((1.0 + s * (FD ** -0.5 + s * (0.5 / FD))) * keep).astype(BF)
            vv = jnp.concatenate([vs[p, :, h * head_dim:(h + 1) * head_dim], ones], axis=1)
            nd[p, h] = dot(w, vv)
            phs[p, h] = features(kt[0, head_rows(h)], rows, weights).astype(BF).T

    sqsend[...] = jnp.zeros_like(sqsend)

    def flat(block):
        return block.reshape(half * rows, head_dim)

    def zrow_of(state):
        block = state[LIN:ONE + 8].astype(F32)
        return jnp.concatenate([block[ONE + 1 - LIN:ONE + 2 - LIN], block[ONE + 2 - LIN:ONE + 3 - LIN, :ONE + 8 - LANES]], axis=1)

    def outer(p):
        @pl.loop(0, cpp)
        def _(j):
            to_seq(fwd.at[p, j], pre.at[p, 0, j], s3, r3.at[p, j], mate).wait_recv()
        live = (iota((span, 1), 0) + me * span < len_ref[p]).astype(F32)
        earlier = jnp.minimum(me * span, len_ref[p]).astype(F32)
        sq = jnp.zeros((sqsend.shape[0], span), F32)
        for h in range(heads):
            state = flat(pre[p, h // half])[(h % half) * rows:(h % half + 1) * rows]
            zr = zrow_of(state)
            zr = jnp.where(iota(zr.shape, 1) == ONE, 0.0, zr)
            zb = jnp.broadcast_to(zr, (head_dim, zr.shape[1])).astype(BF)
            phit = phs[p, h]
            num = dot(phit, state) + nd[p, h, :, :head_dim]
            den = dot(phit[:, :zr.shape[1]], zb, NT) + nd[p, h, :, head_dim:] + earlier
            att = num / den * live
            att_out[p, :, pl.ds(pl.multiple_of(head_of(h) * head_dim, LANES), head_dim)] = att
            sq = sq + dot(jnp.ones((sqsend.shape[0], head_dim), BF), (att * att).astype(BF), NT)
        sqsend[...] = jnp.where(iota(sq.shape, 0) == p, sq, sqsend[...])

        @pl.when(p == npr - 1)
        def _():
            sqgot[fi] = sqsend[...]
            for i in range(1, nf):
                to_feat(sqsend, sqgot.at[fi], s4.at[i], r4.at[fi], lax.rem(fi + i, nf)).start()

    per = FD * FD // nf

    def spread(p, slot, total):
        c = 1 - yi if slot == 0 else yi
        pick = pick_matrix(0, FD * FD, rows).astype(BF)
        for i in range(half):
            h = c * half + i
            mine = total[i * rows:(i + 1) * rows].astype(BF)
            zr = zrow_of(mine)
            zr = jnp.where(iota(zr.shape, 1) == ONE, len_ref[p].astype(F32), zr)
            ztsend[pl.ds(p * heads + h, 1)] = zr
            full = dot(pick, mine).astype(BF)
            for f in range(nf):
                tsend[f, p, h] = full[f * per:(f + 1) * per]
            end = mine[LIN:].astype(F32)
            low_out[p, h] = jnp.concatenate(
                [end[ONE - LIN:ONE - LIN + 1], end[:FD] * FD ** -0.25], axis=0)
        for i in range(1, nf):
            spread_copy(p, c, i).start()
        which = pl.ds(c * half, half)
        quad_out[fi, p, which] = tsend[fi, p, which]

    def spread_copy(p, c, i):
        target = lax.rem(fi + i, nf)
        which = pl.ds(c * half, half)
        return to_feat(tsend.at[target, p, which], quad_out.at[fi, p, which], s5.at[i], r5.at[fi], target)

    def spread_own(p):
        spread(p, 1, flat(up_got[p].astype(F32) + bsum[p].astype(F32) + dn_got[p].astype(F32)))

    def spread_other(p):
        @pl.loop(0, cpp)
        def _(j):
            suf_copy(p, j).wait_recv()
        spread(p, 0, flat(pre[p, 0].astype(F32) + part[p, 0].astype(F32) + suf[p].astype(F32)))

    far = lag * jnp.maximum(zo, last - zo)

    early = (npr - 2) * cpp

    def step(t, _):
        chain(t)
        at((t - early) * 2, inner, cpp)
        done = t - cpp + 1 - turn
        at(done + turn - far, spread_own, cpp)
        at(done - jnp.where(below, lag * last, early), outer, cpp)
        at(done - lag * last, spread_other, cpp)
        return 0

    lax.fori_loop(early, chunks + lag * last + turn, step, 0)

    ztgot[fi] = ztsend[...]
    for i in range(1, nf):
        to_feat(ztsend, ztgot.at[fi], s6.at[i], r6.at[fi], lax.rem(fi + i, nf)).start()

    for i in range(1, nf):
        src = lax.rem(fi + i, nf)
        to_feat(sqsend, sqgot.at[src], s4.at[i], r4.at[src], fpeer).wait_recv()
        to_feat(tsend.at[src], quad_out.at[src], s5.at[i], r5.at[src], fpeer).wait_recv()
        to_feat(ztsend, ztgot.at[src], s6.at[i], r6.at[src], fpeer).wait_recv()
    for i in range(1, nf):
        to_feat(sqsend, sqgot.at[fi], s4.at[i], r4.at[fi], fpeer).wait_send()
        to_feat(tsend.at[fi], quad_out.at[fi], s5.at[i], r5.at[fi], fpeer).wait_send()
        to_feat(ztsend, ztgot.at[fi], s6.at[i], r6.at[fi], fpeer).wait_send()
    to_seq(fwd, fwd, s0, s0, mate).wait_send()
    to_seq(fwd, fwd, s3, s3, mate).wait_send()
    to_seq(bwd, bwd, s7, s7, mate).wait_send()

    @pl.when(above)
    def _():
        to_seq(up_send, up_send, s1, s1, mate).wait_send()

    @pl.when(below)
    def _():
        to_seq(dn_send, dn_send, s2, s2, mate).wait_send()


def finish(cfg, att, sq, quad, low, zt, mine, mixed_out, quad_out, low_out, nq_out, nl_out,
           mixed_buf, quad_buf, sem):
    nf, heads, npr, per = cfg
    span, width = att.shape[1], att.shape[2]
    fi = lax.axis_index("feat")
    squares = sq[0]
    for f in range(1, nf):
        squares = squares + sq[f]
    inv = lax.rsqrt(squares * (1.0 / (nf * width)) + NORM_FLOOR)
    writes = []
    for p in range(npr):
        mask = mine[p, :1]
        for f in range(nf):
            quad_buf[p, f * heads:(f + 1) * heads] = quad[f, p].astype(F32) * (mask * (2.0 * FD) ** -0.5)
        writes.append(pltpu.make_async_copy(quad_buf.at[p], quad_out.at[p], sem.at[0, p]))
        writes[-1].start()
        col = jnp.broadcast_to(inv[p:p + 1], (LANES, span)).T
        for c in range(width // LANES):
            mixed_buf[p, :, c * LANES:(c + 1) * LANES] = (att[p, :, c * LANES:(c + 1) * LANES] * col).astype(BF)
        writes.append(pltpu.make_async_copy(mixed_buf.at[p], mixed_out.at[p], sem.at[1, p]))
        writes[-1].start()
    own_pick = pick_matrix(fi * per, per, ONE + 8).astype(F32)
    lr, lc = iota((FD + 1, ONE + 8), 0), iota((FD + 1, ONE + 8), 1)
    low_pick = jnp.where(lr == 0, (lc == ONE).astype(F32), (lc == LIN - 1 + lr).astype(F32) * FD ** -0.25)
    nl = dot(zt[fi], low_pick, NT, lax.Precision.HIGHEST)
    for f in range(nf):
        nq = dot(zt[f], own_pick, NT, lax.Precision.HIGHEST) * (2.0 * FD) ** -0.5
        for p in range(npr):
            nq_out[p, f * heads:(f + 1) * heads] = nq[p * heads:(p + 1) * heads] * mine[p, :1, :per]
    for p in range(npr):
        nl_out[p] = nl[p * heads:(p + 1) * heads] * mine[p, :1, :FD + 1]
        for h in range(heads):
            low_out[p, :, h, :] = low[p, h] * mine[p, :1]
    for write in writes:
        write.wait()


def body(hidden_in, w_query, w_key, w_value, lengths, owners):
    npr, span, width = hidden_in.shape
    n, nf = lax.axis_size("seq"), lax.axis_size("feat")
    heads = H // nf
    head_dim = width // H
    rows = -(-LIVE_ROWS // 16) * 16
    half_rows = heads // 2 * rows
    cpp, lag, turn = 2, 3, 3
    cfg = (n, nf, npr, span, heads, rows, cpp, lag, turn)
    per = FD * FD // nf
    chunk = (cpp, half_rows // cpp, head_dim)
    dma = pltpu.SemaphoreType.DMA
    vm = pltpu.VMEM
    ph = npr * heads
    out = pl.pallas_call(
        functools.partial(kernel, cfg),
        out_shape=(
            vm((npr, span, heads * head_dim), F32),
            vm((nf, 8, span), F32),
            vm((nf, npr, heads, per, head_dim), BF),
            vm((npr, heads, FD + 1, head_dim), F32),
            vm((nf, ph, ONE + 8), F32),
            vm((npr, 8, LANES), F32),
        ),
        in_specs=[pl.BlockSpec(memory_space=pltpu.HBM)] * 6,
        out_specs=[pl.BlockSpec(memory_space=pltpu.VMEM)] * 6,
        scratch_shapes=[
            vm((npr, span, width), BF),
            vm((width, 2 * LANES + heads * head_dim), BF),
            vm((npr, span, LANES), BF),
            vm((npr, span, LANES), BF),
            vm((npr, span, heads * head_dim), BF),
            vm((2, LANES, span), F32),
            vm((npr, heads, span, rows), BF),
            vm((npr, heads, span, 2 * head_dim), F32),
            vm((npr, 2) + chunk, BF),
            *[vm((npr,) + chunk, BF)] * 7,
            vm((npr, 2) + chunk, BF),
            *[vm((npr,) + chunk, BF)] * 2,
            vm((nf, npr, heads, per, head_dim), BF),
            vm((8, span), F32),
            vm((ph, ONE + 8), F32),
            pltpu.SMEM((npr,), jnp.int32),
            pltpu.SMEM((npr,), jnp.int32),
            dma((npr + 6,)),
            *[dma, dma((npr, cpp))] * 4,
            *[dma((nf,))] * 6,
            dma, dma((npr, cpp)),
        ],
        compiler_params=pltpu.CompilerParams(
            collective_id=0, has_side_effects=True, vmem_limit_bytes=40 * 1024 * 1024
        ),
        name="layer",
    )(*[pltpu.with_memory_space_constraint(a, pltpu.HBM) for a in (lengths, owners, hidden_in, w_query, w_key, w_value)])
    onchip = [pltpu.with_memory_space_constraint(o, pltpu.VMEM) for o in out]
    block = pl.BlockSpec
    mixed, quad, low, nq, nl = pl.pallas_call(
        functools.partial(finish, (nf, heads, npr, per)),
        out_shape=(
            jax.ShapeDtypeStruct((npr, span, heads * head_dim), BF),
            jax.ShapeDtypeStruct((npr, H, per, head_dim), F32),
            jax.ShapeDtypeStruct((npr, FD + 1, heads, head_dim), F32),
            jax.ShapeDtypeStruct((npr, H, per), F32),
            jax.ShapeDtypeStruct((npr, heads, FD + 1), F32),
        ),
        in_specs=[block(memory_space=pltpu.VMEM)] * 6,
        out_specs=[block(memory_space=pl.ANY)] * 2 + [block(memory_space=pltpu.VMEM)] * 3,
        scratch_shapes=[
            vm((npr, span, heads * head_dim), BF),
            vm((npr, H, per, head_dim), F32),
            dma((2, npr)),
        ],
        compiler_params=pltpu.CompilerParams(vmem_limit_bytes=16 * 1024 * 1024),
        name="finish",
    )(*onchip)
    return (mixed, quad[None], jnp.transpose(low, (0, 2, 1, 3))[None], nq[None], nl[None])


def solution(mesh):
    placed = (P(None, "seq", None), P(), P(), P(None, "feat"), P(), P())
    return jax.shard_map(
        body,
        mesh=mesh,
        in_specs=placed,
        out_specs=(
            P(None, "seq", "feat"),
            P("seq", None, None, "feat", None),
            P("seq", None, "feat", None, None),
            P("seq", None, None, "feat"),
            P("seq", None, "feat", None),
        ),
        check_vma=False,
    )
```

```python
import functools

import jax
import jax.numpy as jnp
from jax import lax
from jax.experimental import pallas as pl
from jax.experimental.pallas import tpu as pltpu
from jax.sharding import PartitionSpec as P

H = 16
FD = 16
NORM_FLOOR = 0.0001
LANES = 128
BF = jnp.bfloat16
F32 = jnp.float32
LIN = 128
FAR = 144
ONE = 152
LIVE_ROWS = 153

NN = (((1,), (0,)), ((), ()))
NT = (((1,), (1,)), ((), ()))
TN = (((0,), (0,)), ((), ()))


def dot(a, b, dims=NN, precision=None):
    return lax.dot_general(a, b, dims, preferred_element_type=F32, precision=precision)


def iota(shape, axis):
    return lax.broadcasted_iota(jnp.int32, shape, axis)


def features(t, rows, weights):
    diag, off, lin = weights
    tokens = t.shape[1]
    blocks = [t * t * diag if diag != 1.0 else t * t]
    scaled = t * off if off != 1.0 else t
    for o in range(1, FD // 2):
        blocks.append(scaled * pltpu.roll(t, FD - o, 0))
    blocks.append(t * lin if lin != 1.0 else t)
    blocks.append(scaled[: FD // 2] * t[FD // 2 :])
    blocks.append((iota((rows - ONE, tokens), 0) == 0).astype(F32))
    return jnp.concatenate(blocks, axis=0)


def pick_matrix(first_row, count, rows):
    r = iota((count, rows), 0) + first_row
    c = iota((count, rows), 1)
    i, j = r >> 4, r & 15
    o = (j - i) & 15
    place = jnp.where(
        o < 8, o * FD + i, jnp.where(o == 8, FAR + jnp.minimum(i, j), (FD - o) * FD + j)
    )
    return (place == c)


def kernel(cfg, len_hbm, own_hbm, x_hbm, wq_hbm, wk_hbm, wv_hbm,
           att_out, sqgot, quad_out, low_out, mine_out,
           hid, wall, qs, ks, vs, kt, phs, nd, part, mgot, bsum, up_got, up_send, dn_got, dn_send,
           fwd, pre, bwd, suf, tsend, sqsend, pick, len_ref, own_ref,
           in_sem, s0, r0, s1, r1, s2, r2, s3, r3, s4, r4, s5, r5, s8, s9, s12, r12, s7, r7):
    n, nf, npr, span, heads, rows, cpp, lag, turn, direct = cfg
    relayed = npr - direct
    me, fi = lax.axis_index("seq"), lax.axis_index("feat")
    own = heads * FD
    half = heads // 2
    last = n // 2 - 1
    zo, yi = me // 2, lax.rem(me, 2)
    mate = me + 1 - 2 * yi
    head_dim = vs.shape[2] // heads
    spot = lax.rem(fi * own, LANES)
    hw = half * head_dim
    chunks = npr * cpp
    below, above = zo > 0, zo < last

    def half_cols(c):
        return pl.ds(pl.multiple_of(c * hw, LANES), hw)

    base = pl.multiple_of((fi * own // LANES) * LANES, LANES)
    middle = wall.shape[0] // 2
    parts = (pl.ds(0, middle), pl.ds(middle, middle))

    def first_loads(i):
        r, sems = parts[i], in_sem.at[npr + i]
        mate_cols = half_cols(1 - yi)
        return [
            pltpu.make_async_copy(x_hbm.at[0, :, r], hid.at[0, :, r], sems.at[0]),
            pltpu.make_async_copy(wq_hbm.at[r, pl.ds(base, LANES)], wall.at[r, pl.ds(0, LANES)], sems.at[1]),
            pltpu.make_async_copy(wk_hbm.at[r, pl.ds(base, LANES)], wall.at[r, pl.ds(LANES, LANES)], sems.at[2]),
            pltpu.make_async_copy(wv_hbm.at[r, mate_cols], wall.at[r, pl.ds(2 * LANES, hw)], sems.at[3]),
        ]

    own_load = pltpu.make_async_copy(wv_hbm.at[:, half_cols(yi)], wall.at[:, pl.ds(2 * LANES + hw, hw)], in_sem.at[0, 0])
    small = [
        pltpu.make_async_copy(len_hbm, len_ref, in_sem.at[0, 1]),
        pltpu.make_async_copy(own_hbm, own_ref, in_sem.at[0, 2]),
    ]

    def hid_copy(p):
        return pltpu.make_async_copy(x_hbm.at[p], hid.at[p], in_sem.at[p, 3])

    for i in range(2):
        for load in first_loads(i):
            load.start()
    for load in small:
        load.start()
    own_load.start()

    barrier = pltpu.get_barrier_semaphore()

    def greet(**target):
        pl.semaphore_signal(barrier, 1, device_id=target, device_id_type=pl.DeviceIdType.MESH)

    greet(seq=mate)

    @pl.when(below)
    def _():
        greet(seq=me - 2)

    @pl.when(above)
    def _():
        greet(seq=me + 2)

    for i in range(1, nf):
        greet(feat=lax.rem(fi + i, nf))
        greet(seq=mate, feat=lax.rem(fi + i, nf))

    sqsend[...] = jnp.zeros_like(sqsend)
    pick[...] = pick_matrix(0, FD * FD, rows).astype(BF)
    send_pre, take_pre = below | (yi == 0), below | (yi == 1)
    send_suf, take_suf = above | (yi == 1), above | (yi == 0)

    @pl.when(zo == 0)
    def _():
        up_got[...] = jnp.zeros(up_got.shape, BF)

    @pl.when(zo == last)
    def _():
        dn_got[...] = jnp.zeros(dn_got.shape, BF)

    @pl.when(jnp.logical_not(take_pre))
    def _():
        pre[:, 0] = jnp.zeros((npr,) + pre.shape[2:], BF)

    @pl.when(jnp.logical_not(take_suf))
    def _():
        suf[...] = jnp.zeros(suf.shape, BF)

    def to_seq(src, dst, ssem, rsem, target):
        return pltpu.make_async_remote_copy(
            src_ref=src, dst_ref=dst, send_sem=ssem, recv_sem=rsem,
            device_id={"seq": target}, device_id_type=pl.DeviceIdType.MESH)

    def to_feat(src, dst, ssem, rsem, target):
        return pltpu.make_async_remote_copy(
            src_ref=src, dst_ref=dst, send_sem=ssem, recv_sem=rsem,
            device_id={"feat": target}, device_id_type=pl.DeviceIdType.MESH)

    def to_mates(src, dst, ssem, rsem, target):
        return pltpu.make_async_remote_copy(
            src_ref=src, dst_ref=dst, send_sem=ssem, recv_sem=rsem,
            device_id={"seq": mate, "feat": target}, device_id_type=pl.DeviceIdType.MESH)

    fpeer = lax.rem(fi + 1, nf)

    def swap_copy(p, j):
        return to_seq(part.at[p, 0, j], mgot.at[p, j], s0, r0.at[p, j], mate)

    def up_copy(p, j):
        return to_seq(up_send.at[p, j], up_got.at[p, j], s1, r1.at[p, j], me + 2 * above.astype(jnp.int32) - 2 * (1 - above.astype(jnp.int32)))

    def dn_copy(p, j):
        return to_seq(dn_send.at[p, j], dn_got.at[p, j], s2, r2.at[p, j], me - 2 * below.astype(jnp.int32) + 2 * (1 - below.astype(jnp.int32)))

    def pre_copy(p, j):
        return to_seq(fwd.at[p, j], pre.at[p, 0, j], s3, r3.at[p, j], mate)

    def suf_copy(p, j):
        return to_seq(bwd.at[p, j], suf.at[p, j], s7, r7.at[p, j], mate)

    def live_row(p):
        return ((iota((1, span), 1) + me * span) < len_ref[p]).astype(F32)

    tail = rows - ONE
    weights = (0.5 / FD, 1.0 / FD, FD ** -0.5)

    def sums_of(slot, side, v, live):
        row = iota((tail, LANES), 0)
        ones = jnp.ones((tail, span), BF)
        gap = jnp.zeros((tail, 2 * LANES - ONE - 8), F32)
        sums = []
        for h in range(half):
            phi = (features(kt[side, head_rows(slot + h)], rows, (1.0, 1.0, 1.0)) * live).astype(BF)
            summed = dot(phi, v[:, h * head_dim:(h + 1) * head_dim])
            zh = dot(ones, phi, NT)
            more = jnp.concatenate([zh[:, LANES:ONE + 8], gap], axis=1)
            end = summed[ONE:] + jnp.where(row == 1, zh[:, :LANES], 0.0) + jnp.where(row == 2, more, 0.0)
            sums.append(jnp.concatenate([summed[:ONE], end], axis=0).astype(BF))
        return jnp.concatenate(sums, axis=0).reshape(part.shape[2:])

    def head_of(slot):
        return (1 - yi if slot < half else yi) * half + slot % half

    def head_rows(slot):
        return pl.ds(pl.multiple_of(spot + head_of(slot) * FD, FD), FD)

    def project(p, first):
        cols = slice(0, 2 * LANES + hw)
        if first:
            for load in first_loads(0):
                load.wait()
            head = dot(hid[p, :, :middle], wall[:middle, cols])
            for load in first_loads(1):
                load.wait()
            for later in range(1, npr):
                hid_copy(later).start()
            head = head + dot(hid[p, :, middle:], wall[middle:, cols])
        else:
            hid_copy(p).wait()
            head = dot(hid[p], wall[:, cols])
        k = head[:, LANES:2 * LANES].astype(BF)
        qs[p] = head[:, :LANES].astype(BF)
        ks[p] = k
        slot = lax.rem(p, 2)
        kt[slot] = k.astype(F32).T
        v = head[:, 2 * LANES:].astype(BF)
        vs[p, :, :hw] = v
        if first:
            own_load.wait()
            for load in small:
                load.wait()
        else:
            late(p - 1)
        mine = jnp.concatenate(
            [dot(hid[p, r * span // 2:(r + 1) * span // 2], wall[:, 2 * LANES + hw:]) for r in range(2)], axis=0)
        part[p, 0] = sums_of(0, slot, v, live_row(p))
        vs[p, :, hw:] = mine.astype(BF)
        if first:
            pl.semaphore_wait(barrier, 2 * nf - 1 + below.astype(jnp.int32) + above.astype(jnp.int32))
        for j in range(cpp):
            swap_copy(p, j).start()

    def late(p):
        part[p, 1] = sums_of(half, lax.rem(p, 2), vs[p, :, hw:], live_row(p))

    def pair(k):
        p, j = k // cpp, lax.rem(k, cpp)
        swap_copy(p, j).wait_recv()
        bsum[p, j] = (part[p, 1, j].astype(F32) + mgot[p, j].astype(F32)).astype(BF)

    def take_up(k):
        p, j = k // cpp, lax.rem(k, cpp)

        @pl.when(below)
        def _():
            up_copy(p, j).wait_recv()
        before = up_got[p, j].astype(F32)

        @pl.when(above)
        def _():
            up_send[p, j] = (up_got[p, j].astype(F32) + bsum[p, j].astype(F32)).astype(BF)
            up_copy(p, j).start()
        fwd[p, j] = (before + jnp.where(yi == 0, part[p, 1, j].astype(F32), 0.0)).astype(BF)

        @pl.when(below)
        def _():
            pre_copy(p, j).start()
        pre[p, 1, j] = (before + jnp.where(yi == 1, mgot[p, j].astype(F32), 0.0)).astype(BF)

    def take_down(k):
        p, j = k // cpp, lax.rem(k, cpp)

        @pl.when(above)
        def _():
            dn_copy(p, j).wait_recv()
        after = dn_got[p, j].astype(F32)

        @pl.when(below)
        def _():
            dn_send[p, j] = (dn_got[p, j].astype(F32) + bsum[p, j].astype(F32)).astype(BF)
            dn_copy(p, j).start()
        bwd[p, j] = (after + jnp.where(yi == 1, part[p, 1, j].astype(F32), 0.0)).astype(BF)

        @pl.when(above & (p < relayed))
        def _():
            suf_copy(p, j).start()

    def at(t, body, stride=1):
        @pl.when((t >= 0) & (t < chunks) & (lax.rem(t, stride) == 0))
        def _():
            body(t // stride)

    def chain(t):
        at(t, pair)
        at(t - lag * zo, take_up)
        at(t - lag * (last - zo), take_down)

    project(0, True)

    @pl.loop(1, npr)
    def _(p):
        project(p, False)

        @pl.loop(jnp.maximum(p - 2, 0) * cpp, (p - 1) * cpp)
        def _(t):
            chain(t)

    late(npr - 1)
    for p in range(npr):
        mine_out[p] = jnp.where(iota(mine_out.shape[1:], 0) == 1, len_ref[p].astype(F32), (own_ref[p] == me).astype(F32))

    def inner(p):
        causal = iota((span, span), 0) >= iota((span, span), 1)
        keep = jnp.where(causal, live_row(p), 0.0)
        ones = jnp.ones((span, head_dim), BF)
        lane = iota((1, LANES), 1) // FD
        q, k = qs[p], ks[p].astype(F32)
        kt[0] = q.astype(F32).T
        for h in range(heads):
            mask = (lane == spot // FD + head_of(h)).astype(F32)
            s = dot(q, (k * mask).astype(BF), NT)
            w = ((1.0 + s * (FD ** -0.5 + s * (0.5 / FD))) * keep).astype(BF)
            vv = jnp.concatenate([vs[p, :, h * head_dim:(h + 1) * head_dim], ones], axis=1)
            nd[p, h] = dot(w, vv)
            phs[p, h] = features(kt[0, head_rows(h)], rows, weights).astype(BF).T


    def flat(block):
        return block.reshape(half * rows, head_dim)

    def zrow_of(state):
        block = state[LIN:ONE + 8].astype(F32)
        return jnp.concatenate([block[ONE + 1 - LIN:ONE + 2 - LIN], block[ONE + 2 - LIN:ONE + 3 - LIN, :ONE + 8 - LANES]], axis=1)

    def outer(p, mates):
        live = (iota((span, 1), 0) + me * span < len_ref[p]).astype(F32)
        earlier = jnp.minimum(me * span, len_ref[p]).astype(F32)
        squares = jnp.zeros((span, head_dim), F32)
        for i in range(half):
            slot = i if mates else half + i
            head = (1 - yi if mates else yi) * half + i
            state = pre[p, 0 if mates else 1, i]
            zr = zrow_of(state)
            zr = jnp.where(iota(zr.shape, 1) == ONE, 0.0, zr)
            zb = jnp.broadcast_to(zr, (head_dim, zr.shape[1])).astype(BF)
            phit = phs[p, slot]
            num = dot(phit, state) + nd[p, slot, :, :head_dim]
            den = dot(phit[:, :zr.shape[1]], zb, NT) + nd[p, slot, :, head_dim:] + earlier
            att = num / den * live
            att_out[p, :, pl.ds(pl.multiple_of(head * head_dim, LANES), head_dim)] = att
            squares = squares + att * att
        sq = dot(jnp.ones((sqsend.shape[0], head_dim), BF), squares.astype(BF), NT)
        sqsend[...] += jnp.where(iota(sq.shape, 0) == p, sq, 0.0)

    def outer_own(p):
        outer(p, False)

    def outer_other(p):
        @pl.when(take_pre)
        def _():
            for j in range(cpp):
                pre_copy(p, j).wait_recv()
        outer(p, True)

        @pl.when(p == npr - 1)
        def _():
            sqgot[fi] = sqsend[...]
            for i in range(1, nf):
                to_feat(sqsend, sqgot.at[fi], s4.at[i], r4.at[fi], lax.rem(fi + i, nf)).start()

    per = FD * FD // nf

    def spread(p, c, totals):
        mine = [total.astype(BF) for total in totals]
        full = dot(pick[...], jnp.concatenate(mine, axis=1)).astype(BF)
        zrows = [zrow_of(m) for m in mine]
        fill = jnp.zeros((8 - half, zrows[0].shape[1]), F32)
        zq = dot(jnp.concatenate(zrows + [fill], axis=0).astype(BF), pick[...], NT)
        blank = jnp.zeros((8, head_dim - per), F32)
        for f in range(nf):
            for i in range(half):
                tsend[f, p, c, i * per:(i + 1) * per] = full[f * per:(f + 1) * per, i * head_dim:(i + 1) * head_dim]
            tsend[f, p, c, half * per:] = jnp.concatenate([zq[:, f * per:(f + 1) * per], blank], axis=1).astype(BF)
        last_one = p >= relayed

        @pl.when(jnp.logical_not(last_one))
        def _():
            for i in range(1, nf):
                target = lax.rem(fi + i, nf)
                to_feat(tsend.at[target, p, c], quad_out.at[fi, p, c], s5.at[i], r5.at[fi], target).start()
        quad_out[fi, p, c] = tsend[fi, p, c]
        for i in range(half):
            end = mine[i][LIN:].astype(F32)
            lows = end[:FD] * FD ** -0.25
            count = jnp.where(iota((1, 1), 0) == 0, len_ref[p].astype(F32), 0.0)
            zlow = jnp.concatenate([count, end[ONE + 2 - LIN:ONE + 3 - LIN, :FD] * FD ** -0.25, jnp.zeros((1, head_dim - FD - 1), F32)], axis=1)
            low_out[p, c * half + i] = jnp.concatenate(
                [end[ONE - LIN:ONE - LIN + 1], lows, zlow, jnp.zeros((6, head_dim), F32)], axis=0)


    def low_copy(p, c):
        which = pl.ds(c * half, half)
        return to_seq(low_out.at[p, which], low_out.at[p, which], s12, r12, mate)

    def spread_own(p):
        spread(p, yi, [up_got[p, j].astype(F32) + bsum[p, j].astype(F32) + dn_got[p, j].astype(F32) for j in range(cpp)])

    def spread_other(p):
        @pl.when(take_suf)
        def _():
            for j in range(cpp):
                suf_copy(p, j).wait_recv()
        spread(p, 1 - yi, [pre[p, 0, j].astype(F32) + part[p, 0, j].astype(F32) + suf[p, j].astype(F32) for j in range(cpp)])

    def held_pre(k):
        pre_copy(k // cpp, lax.rem(k, cpp)).start()

    def held_suf(k):
        @pl.when(k < relayed * cpp)
        def _():
            suf_copy(k // cpp, lax.rem(k, cpp)).start()

    early = (npr - 2) * cpp
    reach = max(lag * last, early + npr)
    far = jnp.maximum(lag * jnp.maximum(zo, last - zo), early)

    hold = early

    def step(t, _):
        chain(t)
        at(t - jnp.where(jnp.logical_not(below) & send_pre, hold, chunks + t), held_pre)
        at(t - jnp.where(jnp.logical_not(above) & send_suf, hold, chunks + t), held_suf)
        at((t - early) * 2, inner, cpp)
        base_own = jnp.where(below, reach, early + npr)
        back = t - cpp + 1
        at(back - base_own - turn, outer_other, cpp)
        at(back - far, spread_own, cpp)
        at(back - base_own, outer_own, cpp)
        mine = back - reach - turn
        at(jnp.where(mine < relayed * cpp, mine, -1), spread_other, cpp)
        return 0

    lax.fori_loop(early, chunks + reach + turn, step, 0)

    ends, starts = pl.ds(relayed, direct), pl.ds(0, relayed)
    own_side, mate_side = pl.ds(yi * half, half), pl.ds((1 - yi) * half, half)
    for i in range(1, nf):
        src = lax.rem(fi + i, nf)
        to_feat(sqsend, sqgot.at[src], s4.at[i], r4.at[src], fpeer).wait_recv()
        to_feat(tsend.at[src], quad_out.at[src], s5.at[i], r5.at[src], fpeer).wait_recv()
    for i in range(1, nf):
        to_feat(sqsend, sqgot.at[fi], s4.at[i], r4.at[fi], fpeer).wait_send()
        to_feat(tsend.at[fi, starts], quad_out.at[fi, starts], s5.at[i], r5.at[fi], fpeer).wait_send()
    to_seq(fwd, fwd, s0, s0, mate).wait_send()

    @pl.when(send_pre)
    def _():
        to_seq(fwd, fwd, s3, s3, mate).wait_send()

    @pl.when(send_suf)
    def _():
        to_seq(bwd.at[starts], bwd.at[starts], s7, s7, mate).wait_send()

    @pl.when(above)
    def _():
        to_seq(up_send, up_send, s1, s1, mate).wait_send()

    @pl.when(below)
    def _():
        to_seq(dn_send, dn_send, s2, s2, mate).wait_send()


def finish(cfg, att, sq, quad, low, mine, mixed_out, quad_out, low_out, nq_out, nl_out,
           mixed_buf, quad_buf, sem):
    nf, heads, npr, per = cfg
    span, width = att.shape[1], att.shape[2]
    half = heads // 2
    scale = (2.0 * FD) ** -0.5
    squares = sq[0]
    for f in range(1, nf):
        squares = squares + sq[f]
    inv = lax.rsqrt(squares * (1.0 / (nf * width)) + NORM_FLOOR)
    writes = []
    for p in range(npr):
        mask = mine[p, :1] * scale
        for f in range(nf):
            for c in range(2):
                block = quad[f, p, c].astype(F32) * mask
                for i in range(half):
                    quad_buf[p, f * heads + c * half + i] = block[i * per:(i + 1) * per]
                nq_out[p, f * heads + c * half:f * heads + (c + 1) * half] = block[half * per:half * per + half, :per]
        writes.append(pltpu.make_async_copy(quad_buf.at[p], quad_out.at[p], sem.at[0, p]))
        writes[-1].start()
        col = jnp.broadcast_to(inv[p:p + 1], (LANES, span)).T
        for c in range(width // LANES):
            mixed_buf[p, :, c * LANES:(c + 1) * LANES] = (att[p, :, c * LANES:(c + 1) * LANES] * col).astype(BF)
        writes.append(pltpu.make_async_copy(mixed_buf.at[p], mixed_out.at[p], sem.at[1, p]))
        writes[-1].start()
    for p in range(npr):
        for h in range(heads):
            full = low[p, h] * mine[p, :1]
            low_out[p, :, h, :] = full[:FD + 1]
            nl_out[p, h:h + 1] = full[FD + 1:FD + 2, :FD + 1]
    for write in writes:
        write.wait()


def body(hidden_in, w_query, w_key, w_value, lengths, owners):
    npr, span, width = hidden_in.shape
    n, nf = lax.axis_size("seq"), lax.axis_size("feat")
    heads = H // nf
    head_dim = width // H
    rows = -(-LIVE_ROWS // 16) * 16
    half_rows = heads // 2 * rows
    cpp, lag, turn = heads // 2, 3, 3
    cfg = (n, nf, npr, span, heads, rows, cpp, lag, turn, 0)
    per = FD * FD // nf
    chunk = (cpp, half_rows // cpp, head_dim)
    dma = pltpu.SemaphoreType.DMA
    vm = pltpu.VMEM
    out = pl.pallas_call(
        functools.partial(kernel, cfg),
        out_shape=(
            vm((npr, span, heads * head_dim), F32),
            vm((nf, 8, span), F32),
            vm((nf, npr, 2, heads // 2 * per + 8, head_dim), BF),
            vm((npr, heads, 24, head_dim), F32),
            vm((npr, 8, LANES), F32),
        ),
        in_specs=[pl.BlockSpec(memory_space=pltpu.HBM)] * 6,
        out_specs=[pl.BlockSpec(memory_space=pltpu.VMEM)] * 5,
        scratch_shapes=[
            vm((npr, span, width), BF),
            vm((width, 2 * LANES + heads * head_dim), BF),
            vm((npr, span, LANES), BF),
            vm((npr, span, LANES), BF),
            vm((npr, span, heads * head_dim), BF),
            vm((2, LANES, span), F32),
            vm((npr, heads, span, rows), BF),
            vm((npr, heads, span, 2 * head_dim), F32),
            vm((npr, 2) + chunk, BF),
            *[vm((npr,) + chunk, BF)] * 7,
            vm((npr, 2) + chunk, BF),
            *[vm((npr,) + chunk, BF)] * 2,
            vm((nf, npr, 2, heads // 2 * per + 8, head_dim), BF),
            vm((8, span), F32),
            vm((FD * FD, rows), BF),
            pltpu.SMEM((npr,), jnp.int32),
            pltpu.SMEM((npr,), jnp.int32),
            dma((npr + 2, 4)),
            *[dma, dma((npr, cpp))] * 4,
            *[dma((nf,))] * 6,
            dma, dma,
            dma, dma((npr, cpp)),
        ],
        compiler_params=pltpu.CompilerParams(
            collective_id=0, has_side_effects=True, vmem_limit_bytes=40 * 1024 * 1024
        ),
        name="layer",
    )(*[pltpu.with_memory_space_constraint(a, pltpu.HBM) for a in (lengths, owners, hidden_in, w_query, w_key, w_value)])
    onchip = [pltpu.with_memory_space_constraint(o, pltpu.VMEM) for o in out]
    block = pl.BlockSpec
    mixed, quad, low, nq, nl = pl.pallas_call(
        functools.partial(finish, (nf, heads, npr, per)),
        out_shape=(
            jax.ShapeDtypeStruct((npr, span, heads * head_dim), BF),
            jax.ShapeDtypeStruct((npr, H, per, head_dim), F32),
            jax.ShapeDtypeStruct((npr, FD + 1, heads, head_dim), F32),
            jax.ShapeDtypeStruct((npr, H, per), F32),
            jax.ShapeDtypeStruct((npr, heads, FD + 1), F32),
        ),
        in_specs=[block(memory_space=pltpu.VMEM)] * 5,
        out_specs=[block(memory_space=pl.ANY)] * 2 + [block(memory_space=pltpu.VMEM)] * 3,
        scratch_shapes=[
            vm((npr, span, heads * head_dim), BF),
            vm((npr, H, per, head_dim), F32),
            dma((2, npr)),
        ],
        compiler_params=pltpu.CompilerParams(vmem_limit_bytes=16 * 1024 * 1024),
        name="finish",
    )(*onchip)
    return (mixed, quad[None], jnp.transpose(low, (0, 2, 1, 3))[None], nq[None], nl[None])


def solution(mesh):
    placed = (P(None, "seq", None), P(), P(), P(None, "feat"), P(), P())
    return jax.shard_map(
        body,
        mesh=mesh,
        in_specs=placed,
        out_specs=(
            P(None, "seq", "feat"),
            P("seq", None, None, "feat", None),
            P("seq", None, "feat", None, None),
            P("seq", None, None, "feat"),
            P("seq", None, "feat", None),
        ),
        check_vma=False,
    )
```

```python
import functools

import jax
import jax.numpy as jnp
from jax import lax
from jax.experimental import pallas as pl
from jax.experimental.pallas import tpu as pltpu
from jax.sharding import PartitionSpec as P

H = 16
FD = 16
NORM_FLOOR = 0.0001
LANES = 128
BF = jnp.bfloat16
F32 = jnp.float32
LIN = 128
FAR = 144
ONE = 152
LIVE_ROWS = 153

NN = (((1,), (0,)), ((), ()))
NT = (((1,), (1,)), ((), ()))
TN = (((0,), (0,)), ((), ()))


def dot(a, b, dims=NN, precision=None):
    return lax.dot_general(a, b, dims, preferred_element_type=F32, precision=precision)


def iota(shape, axis):
    return lax.broadcasted_iota(jnp.int32, shape, axis)


def features(t, rows, weights):
    diag, off, lin = weights
    tokens = t.shape[1]
    blocks = [t * t * diag if diag != 1.0 else t * t]
    scaled = t * off if off != 1.0 else t
    for o in range(1, FD // 2):
        blocks.append(scaled * pltpu.roll(t, FD - o, 0))
    blocks.append(t * lin if lin != 1.0 else t)
    blocks.append(scaled[: FD // 2] * t[FD // 2 :])
    blocks.append((iota((rows - ONE, tokens), 0) == 0).astype(F32))
    return jnp.concatenate(blocks, axis=0)


def pick_matrix(first_row, count, rows):
    r = iota((count, rows), 0) + first_row
    c = iota((count, rows), 1)
    i, j = r >> 4, r & 15
    o = (j - i) & 15
    place = jnp.where(
        o < 8, o * FD + i, jnp.where(o == 8, FAR + jnp.minimum(i, j), (FD - o) * FD + j)
    )
    return (place == c)


def kernel(cfg, len_hbm, own_hbm, x_hbm, wq_hbm, wk_hbm, wv_hbm,
           att_out, sqgot, quad_out, low_out, mine_out,
           hid, wall, qs, ks, vs, kt, phs, nd, part, mgot, bsum, up_got, up_send, dn_got, dn_send,
           fwd, pre, bwd, suf, tsend, sqsend, pick, len_ref, own_ref,
           in_sem, s0, r0, s1, r1, s2, r2, s3, r3, s4, r4, s5, r5, s8, s9, s12, r12, s7, r7):
    n, nf, npr, span, heads, rows, cpp, lag, turn, direct = cfg
    relayed = npr - direct
    me, fi = lax.axis_index("seq"), lax.axis_index("feat")
    own = heads * FD
    half = heads // 2
    last = n // 2 - 1
    zo, yi = me // 2, lax.rem(me, 2)
    mate = me + 1 - 2 * yi
    head_dim = vs.shape[2] // heads
    spot = lax.rem(fi * own, LANES)
    hw = half * head_dim
    chunks = npr * cpp
    below, above = zo > 0, zo < last

    def half_cols(c):
        return pl.ds(pl.multiple_of(c * hw, LANES), hw)

    base = pl.multiple_of((fi * own // LANES) * LANES, LANES)
    middle = wall.shape[0] // 2
    parts = (pl.ds(0, middle), pl.ds(middle, middle))

    def first_loads(i):
        r, sems = parts[i], in_sem.at[npr + i]
        mate_cols = half_cols(1 - yi)
        return [
            pltpu.make_async_copy(x_hbm.at[0, :, r], hid.at[0, :, r], sems.at[0]),
            pltpu.make_async_copy(wq_hbm.at[r, pl.ds(base, LANES)], wall.at[r, pl.ds(0, LANES)], sems.at[1]),
            pltpu.make_async_copy(wk_hbm.at[r, pl.ds(base, LANES)], wall.at[r, pl.ds(LANES, LANES)], sems.at[2]),
            pltpu.make_async_copy(wv_hbm.at[r, mate_cols], wall.at[r, pl.ds(2 * LANES, hw)], sems.at[3]),
        ]

    own_load = pltpu.make_async_copy(wv_hbm.at[:, half_cols(yi)], wall.at[:, pl.ds(2 * LANES + hw, hw)], in_sem.at[0, 0])
    small = [
        pltpu.make_async_copy(len_hbm, len_ref, in_sem.at[0, 1]),
        pltpu.make_async_copy(own_hbm, own_ref, in_sem.at[0, 2]),
    ]

    def hid_copy(p):
        return pltpu.make_async_copy(x_hbm.at[p], hid.at[p], in_sem.at[p, 3])

    for i in range(2):
        for load in first_loads(i):
            load.start()
    for load in small:
        load.start()
    own_load.start()

    barrier = pltpu.get_barrier_semaphore()

    def greet(**target):
        pl.semaphore_signal(barrier, 1, device_id=target, device_id_type=pl.DeviceIdType.MESH)

    greet(seq=mate)

    @pl.when(below)
    def _():
        greet(seq=me - 2)

    @pl.when(above)
    def _():
        greet(seq=me + 2)

    for i in range(1, nf):
        greet(feat=lax.rem(fi + i, nf))
        greet(seq=mate, feat=lax.rem(fi + i, nf))

    sqsend[...] = jnp.zeros_like(sqsend)
    pick[...] = pick_matrix(0, FD * FD, rows).astype(BF)
    send_pre, take_pre = below | (yi == 0), below | (yi == 1)
    send_suf, take_suf = above | (yi == 1), above | (yi == 0)

    @pl.when(zo == 0)
    def _():
        up_got[...] = jnp.zeros(up_got.shape, BF)

    @pl.when(zo == last)
    def _():
        dn_got[...] = jnp.zeros(dn_got.shape, BF)

    @pl.when(jnp.logical_not(take_pre))
    def _():
        pre[:, 0] = jnp.zeros((npr,) + pre.shape[2:], BF)

    @pl.when(jnp.logical_not(take_suf))
    def _():
        suf[...] = jnp.zeros(suf.shape, BF)

    def to_seq(src, dst, ssem, rsem, target):
        return pltpu.make_async_remote_copy(
            src_ref=src, dst_ref=dst, send_sem=ssem, recv_sem=rsem,
            device_id={"seq": target}, device_id_type=pl.DeviceIdType.MESH)

    def to_feat(src, dst, ssem, rsem, target):
        return pltpu.make_async_remote_copy(
            src_ref=src, dst_ref=dst, send_sem=ssem, recv_sem=rsem,
            device_id={"feat": target}, device_id_type=pl.DeviceIdType.MESH)

    def to_mates(src, dst, ssem, rsem, target):
        return pltpu.make_async_remote_copy(
            src_ref=src, dst_ref=dst, send_sem=ssem, recv_sem=rsem,
            device_id={"seq": mate, "feat": target}, device_id_type=pl.DeviceIdType.MESH)

    fpeer = lax.rem(fi + 1, nf)

    def swap_copy(p, j):
        return to_seq(part.at[p, 0, j], mgot.at[p, j], s0, r0.at[p, j], mate)

    def up_copy(p, j):
        return to_seq(up_send.at[p, j], up_got.at[p, j], s1, r1.at[p, j], me + 2 * above.astype(jnp.int32) - 2 * (1 - above.astype(jnp.int32)))

    def dn_copy(p, j):
        return to_seq(dn_send.at[p, j], dn_got.at[p, j], s2, r2.at[p, j], me - 2 * below.astype(jnp.int32) + 2 * (1 - below.astype(jnp.int32)))

    def pre_copy(p, j):
        return to_seq(fwd.at[p, j], pre.at[p, 0, j], s3, r3.at[p, j], mate)

    def suf_copy(p, j):
        return to_seq(bwd.at[p, j], suf.at[p, j], s7, r7.at[p, j], mate)

    def live_row(p):
        return ((iota((1, span), 1) + me * span) < len_ref[p]).astype(F32)

    tail = rows - ONE
    weights = (0.5 / FD, 1.0 / FD, FD ** -0.5)

    def sums_of(slot, side, v, live):
        row = iota((tail, LANES), 0)
        ones = jnp.ones((tail, span), BF)
        gap = jnp.zeros((tail, 2 * LANES - ONE - 8), F32)
        sums = []
        for h in range(half):
            phi = (features(kt[side, head_rows(slot + h)], rows, (1.0, 1.0, 1.0)) * live).astype(BF)
            summed = dot(phi, v[:, h * head_dim:(h + 1) * head_dim])
            zh = dot(ones, phi, NT)
            more = jnp.concatenate([zh[:, LANES:ONE + 8], gap], axis=1)
            end = summed[ONE:] + jnp.where(row == 1, zh[:, :LANES], 0.0) + jnp.where(row == 2, more, 0.0)
            sums.append(jnp.concatenate([summed[:ONE], end], axis=0).astype(BF))
        return jnp.concatenate(sums, axis=0).reshape(part.shape[2:])

    def head_of(slot):
        return (1 - yi if slot < half else yi) * half + slot % half

    def head_rows(slot):
        return pl.ds(pl.multiple_of(spot + head_of(slot) * FD, FD), FD)

    def project(p, first):
        cols = slice(0, 2 * LANES + hw)
        if first:
            for load in first_loads(0):
                load.wait()
            head = dot(hid[p, :, :middle], wall[:middle, cols])
            for load in first_loads(1):
                load.wait()
            for later in range(1, npr):
                hid_copy(later).start()
            head = head + dot(hid[p, :, middle:], wall[middle:, cols])
        else:
            hid_copy(p).wait()
            head = dot(hid[p], wall[:, cols])
        k = head[:, LANES:2 * LANES].astype(BF)
        qs[p] = head[:, :LANES].astype(BF)
        ks[p] = k
        slot = lax.rem(p, 2)
        kt[slot] = k.astype(F32).T
        v = head[:, 2 * LANES:].astype(BF)
        vs[p, :, :hw] = v
        mine_cols = slice(2 * LANES + hw, 2 * LANES + 2 * hw)

        def own_values():
            return jnp.concatenate(
                [dot(hid[p, r * span // 2:(r + 1) * span // 2], wall[:, mine_cols]) for r in range(2)], axis=0).astype(BF)

        if first:
            for load in small:
                load.wait()
        else:
            late(p - 1)
            mine = own_values()
        part[p, 0] = sums_of(0, slot, v, live_row(p))
        if first:
            pl.semaphore_wait(barrier, 2 * nf - 1 + below.astype(jnp.int32) + above.astype(jnp.int32))
        for j in range(cpp):
            swap_copy(p, j).start()
        if first:
            own_load.wait()
            mine = own_values()
        vs[p, :, hw:] = mine

    def late(p):
        part[p, 1] = sums_of(half, lax.rem(p, 2), vs[p, :, hw:], live_row(p))

    def pair(k):
        p, j = k // cpp, lax.rem(k, cpp)
        swap_copy(p, j).wait_recv()
        bsum[p, j] = (part[p, 1, j].astype(F32) + mgot[p, j].astype(F32)).astype(BF)

    def take_up(k):
        p, j = k // cpp, lax.rem(k, cpp)

        @pl.when(below)
        def _():
            up_copy(p, j).wait_recv()
        before = up_got[p, j].astype(F32)

        @pl.when(above)
        def _():
            up_send[p, j] = (up_got[p, j].astype(F32) + bsum[p, j].astype(F32)).astype(BF)
            up_copy(p, j).start()
        fwd[p, j] = (before + jnp.where(yi == 0, part[p, 1, j].astype(F32), 0.0)).astype(BF)

        @pl.when(below)
        def _():
            pre_copy(p, j).start()
        pre[p, 1, j] = (before + jnp.where(yi == 1, mgot[p, j].astype(F32), 0.0)).astype(BF)

    def take_down(k):
        p, j = k // cpp, lax.rem(k, cpp)

        @pl.when(above)
        def _():
            dn_copy(p, j).wait_recv()
        after = dn_got[p, j].astype(F32)

        @pl.when(below)
        def _():
            dn_send[p, j] = (dn_got[p, j].astype(F32) + bsum[p, j].astype(F32)).astype(BF)
            dn_copy(p, j).start()
        bwd[p, j] = (after + jnp.where(yi == 1, part[p, 1, j].astype(F32), 0.0)).astype(BF)

        @pl.when(above & (p < relayed))
        def _():
            suf_copy(p, j).start()

    def at(t, body, stride=1):
        @pl.when((t >= 0) & (t < chunks) & (lax.rem(t, stride) == 0))
        def _():
            body(t // stride)

    def chain(t):
        at(t, pair)
        at(t - lag * zo, take_up)
        at(t - lag * (last - zo), take_down)

    project(0, True)

    @pl.loop(1, npr)
    def _(p):
        project(p, False)

        @pl.loop(jnp.maximum(p - 2, 0) * cpp, (p - 1) * cpp)
        def _(t):
            chain(t)

    late(npr - 1)
    for p in range(npr):
        mine_out[p] = jnp.where(iota(mine_out.shape[1:], 0) == 1, len_ref[p].astype(F32), (own_ref[p] == me).astype(F32))

    def inner(p):
        causal = iota((span, span), 0) >= iota((span, span), 1)
        keep = jnp.where(causal, live_row(p), 0.0)
        ones = jnp.ones((span, head_dim), BF)
        lane = iota((1, LANES), 1) // FD
        q, k = qs[p], ks[p].astype(F32)
        kt[0] = q.astype(F32).T
        for h in range(heads):
            mask = (lane == spot // FD + head_of(h)).astype(F32)
            s = dot(q, (k * mask).astype(BF), NT)
            w = ((1.0 + s * (FD ** -0.5 + s * (0.5 / FD))) * keep).astype(BF)
            vv = jnp.concatenate([vs[p, :, h * head_dim:(h + 1) * head_dim], ones], axis=1)
            nd[p, h] = dot(w, vv)
            phs[p, h] = features(kt[0, head_rows(h)], rows, weights).astype(BF).T


    def flat(block):
        return block.reshape(half * rows, head_dim)

    def zrow_of(state):
        block = state[LIN:ONE + 8].astype(F32)
        return jnp.concatenate([block[ONE + 1 - LIN:ONE + 2 - LIN], block[ONE + 2 - LIN:ONE + 3 - LIN, :ONE + 8 - LANES]], axis=1)

    def outer(p, mates):
        live = (iota((span, 1), 0) + me * span < len_ref[p]).astype(F32)
        earlier = jnp.minimum(me * span, len_ref[p]).astype(F32)
        squares = jnp.zeros((span, head_dim), F32)
        for i in range(half):
            slot = i if mates else half + i
            head = (1 - yi if mates else yi) * half + i
            state = pre[p, 0 if mates else 1, i]
            zr = zrow_of(state)
            zr = jnp.where(iota(zr.shape, 1) == ONE, 0.0, zr)
            zb = jnp.broadcast_to(zr, (head_dim, zr.shape[1])).astype(BF)
            phit = phs[p, slot]
            num = dot(phit, state) + nd[p, slot, :, :head_dim]
            den = dot(phit[:, :zr.shape[1]], zb, NT) + nd[p, slot, :, head_dim:] + earlier
            att = num / den * live
            att_out[p, :, pl.ds(pl.multiple_of(head * head_dim, LANES), head_dim)] = att
            squares = squares + att * att
        sq = dot(jnp.ones((sqsend.shape[0], head_dim), BF), squares.astype(BF), NT)
        sqsend[...] += jnp.where(iota(sq.shape, 0) == p, sq, 0.0)

    def outer_own(p):
        outer(p, False)

    def outer_other(p):
        @pl.when(take_pre)
        def _():
            for j in range(cpp):
                pre_copy(p, j).wait_recv()
        outer(p, True)

        @pl.when(p == npr - 1)
        def _():
            sqgot[fi] = sqsend[...]
            for i in range(1, nf):
                to_feat(sqsend, sqgot.at[fi], s4.at[i], r4.at[fi], lax.rem(fi + i, nf)).start()

    per = FD * FD // nf

    def spread(p, c, totals):
        mine = [total.astype(BF) for total in totals]
        full = dot(pick[...], jnp.concatenate(mine, axis=1)).astype(BF)
        zrows = [zrow_of(m) for m in mine]
        fill = jnp.zeros((8 - half, zrows[0].shape[1]), F32)
        zq = dot(jnp.concatenate(zrows + [fill], axis=0).astype(BF), pick[...], NT)
        blank = jnp.zeros((8, head_dim - per), F32)
        for f in range(nf):
            for i in range(half):
                tsend[f, p, c, i * per:(i + 1) * per] = full[f * per:(f + 1) * per, i * head_dim:(i + 1) * head_dim]
            tsend[f, p, c, half * per:] = jnp.concatenate([zq[:, f * per:(f + 1) * per], blank], axis=1).astype(BF)
        last_one = p >= relayed

        @pl.when(jnp.logical_not(last_one))
        def _():
            for i in range(1, nf):
                target = lax.rem(fi + i, nf)
                to_feat(tsend.at[target, p, c], quad_out.at[fi, p, c], s5.at[i], r5.at[fi], target).start()
        quad_out[fi, p, c] = tsend[fi, p, c]
        for i in range(half):
            end = mine[i][LIN:].astype(F32)
            lows = end[:FD] * FD ** -0.25
            count = jnp.where(iota((1, 1), 0) == 0, len_ref[p].astype(F32), 0.0)
            zlow = jnp.concatenate([count, end[ONE + 2 - LIN:ONE + 3 - LIN, :FD] * FD ** -0.25, jnp.zeros((1, head_dim - FD - 1), F32)], axis=1)
            low_out[p, c * half + i] = jnp.concatenate(
                [end[ONE - LIN:ONE - LIN + 1], lows, zlow, jnp.zeros((6, head_dim), F32)], axis=0)


    def low_copy(p, c):
        which = pl.ds(c * half, half)
        return to_seq(low_out.at[p, which], low_out.at[p, which], s12, r12, mate)

    def spread_own(p):
        spread(p, yi, [up_got[p, j].astype(F32) + bsum[p, j].astype(F32) + dn_got[p, j].astype(F32) for j in range(cpp)])

    def spread_other(p):
        @pl.when(take_suf)
        def _():
            for j in range(cpp):
                suf_copy(p, j).wait_recv()
        spread(p, 1 - yi, [pre[p, 0, j].astype(F32) + part[p, 0, j].astype(F32) + suf[p, j].astype(F32) for j in range(cpp)])

    def held_pre(k):
        pre_copy(k // cpp, lax.rem(k, cpp)).start()

    def held_suf(k):
        @pl.when(k < relayed * cpp)
        def _():
            suf_copy(k // cpp, lax.rem(k, cpp)).start()

    early = (npr - 2) * cpp
    reach = max(lag * last, early + npr)
    far = jnp.maximum(lag * jnp.maximum(zo, last - zo), early)

    hold = early

    def step(t, _):
        chain(t)
        at(t - jnp.where(jnp.logical_not(below) & send_pre, hold, chunks + t), held_pre)
        at(t - jnp.where(jnp.logical_not(above) & send_suf, hold, chunks + t), held_suf)
        at((t - early) * 2, inner, cpp)
        base_own = jnp.where(below, reach, early + npr)
        back = t - cpp + 1
        at(back - base_own - turn, outer_other, cpp)
        at(back - far, spread_own, cpp)
        at(back - base_own, outer_own, cpp)
        mine = back - reach - turn
        at(jnp.where(mine < relayed * cpp, mine, -1), spread_other, cpp)
        return 0

    lax.fori_loop(early, chunks + reach + turn, step, 0)

    ends, starts = pl.ds(relayed, direct), pl.ds(0, relayed)
    own_side, mate_side = pl.ds(yi * half, half), pl.ds((1 - yi) * half, half)
    for i in range(1, nf):
        src = lax.rem(fi + i, nf)
        to_feat(sqsend, sqgot.at[src], s4.at[i], r4.at[src], fpeer).wait_recv()
        to_feat(tsend.at[src], quad_out.at[src], s5.at[i], r5.at[src], fpeer).wait_recv()
    for i in range(1, nf):
        to_feat(sqsend, sqgot.at[fi], s4.at[i], r4.at[fi], fpeer).wait_send()
        to_feat(tsend.at[fi, starts], quad_out.at[fi, starts], s5.at[i], r5.at[fi], fpeer).wait_send()
    to_seq(fwd, fwd, s0, s0, mate).wait_send()

    @pl.when(send_pre)
    def _():
        to_seq(fwd, fwd, s3, s3, mate).wait_send()

    @pl.when(send_suf)
    def _():
        to_seq(bwd.at[starts], bwd.at[starts], s7, s7, mate).wait_send()

    @pl.when(above)
    def _():
        to_seq(up_send, up_send, s1, s1, mate).wait_send()

    @pl.when(below)
    def _():
        to_seq(dn_send, dn_send, s2, s2, mate).wait_send()


def finish(cfg, att, sq, quad, low, mine, mixed_out, quad_out, low_out, nq_out, nl_out,
           mixed_buf, quad_buf, sem):
    nf, heads, npr, per = cfg
    span, width = att.shape[1], att.shape[2]
    half = heads // 2
    scale = (2.0 * FD) ** -0.5
    squares = sq[0]
    for f in range(1, nf):
        squares = squares + sq[f]
    inv = lax.rsqrt(squares * (1.0 / (nf * width)) + NORM_FLOOR)
    writes = []
    for p in range(npr):
        mask = mine[p, :1] * scale
        for f in range(nf):
            for c in range(2):
                block = quad[f, p, c].astype(F32) * mask
                for i in range(half):
                    quad_buf[p, f * heads + c * half + i] = block[i * per:(i + 1) * per]
                nq_out[p, f * heads + c * half:f * heads + (c + 1) * half] = block[half * per:half * per + half, :per]
        writes.append(pltpu.make_async_copy(quad_buf.at[p], quad_out.at[p], sem.at[0, p]))
        writes[-1].start()
        col = jnp.broadcast_to(inv[p:p + 1], (LANES, span)).T
        for c in range(width // LANES):
            mixed_buf[p, :, c * LANES:(c + 1) * LANES] = (att[p, :, c * LANES:(c + 1) * LANES] * col).astype(BF)
        writes.append(pltpu.make_async_copy(mixed_buf.at[p], mixed_out.at[p], sem.at[1, p]))
        writes[-1].start()
    for p in range(npr):
        for h in range(heads):
            full = low[p, h] * mine[p, :1]
            low_out[p, :, h, :] = full[:FD + 1]
            nl_out[p, h:h + 1] = full[FD + 1:FD + 2, :FD + 1]
    for write in writes:
        write.wait()


def body(hidden_in, w_query, w_key, w_value, lengths, owners):
    npr, span, width = hidden_in.shape
    n, nf = lax.axis_size("seq"), lax.axis_size("feat")
    heads = H // nf
    head_dim = width // H
    rows = -(-LIVE_ROWS // 16) * 16
    half_rows = heads // 2 * rows
    cpp, lag, turn = heads // 2, 3, 3
    cfg = (n, nf, npr, span, heads, rows, cpp, lag, turn, 0)
    per = FD * FD // nf
    chunk = (cpp, half_rows // cpp, head_dim)
    dma = pltpu.SemaphoreType.DMA
    vm = pltpu.VMEM
    out = pl.pallas_call(
        functools.partial(kernel, cfg),
        out_shape=(
            vm((npr, span, heads * head_dim), F32),
            vm((nf, 8, span), F32),
            vm((nf, npr, 2, heads // 2 * per + 8, head_dim), BF),
            vm((npr, heads, 24, head_dim), F32),
            vm((npr, 8, LANES), F32),
        ),
        in_specs=[pl.BlockSpec(memory_space=pltpu.HBM)] * 6,
        out_specs=[pl.BlockSpec(memory_space=pltpu.VMEM)] * 5,
        scratch_shapes=[
            vm((npr, span, width), BF),
            vm((width, 2 * LANES + heads * head_dim), BF),
            vm((npr, span, LANES), BF),
            vm((npr, span, LANES), BF),
            vm((npr, span, heads * head_dim), BF),
            vm((2, LANES, span), F32),
            vm((npr, heads, span, rows), BF),
            vm((npr, heads, span, 2 * head_dim), F32),
            vm((npr, 2) + chunk, BF),
            *[vm((npr,) + chunk, BF)] * 7,
            vm((npr, 2) + chunk, BF),
            *[vm((npr,) + chunk, BF)] * 2,
            vm((nf, npr, 2, heads // 2 * per + 8, head_dim), BF),
            vm((8, span), F32),
            vm((FD * FD, rows), BF),
            pltpu.SMEM((npr,), jnp.int32),
            pltpu.SMEM((npr,), jnp.int32),
            dma((npr + 2, 4)),
            *[dma, dma((npr, cpp))] * 4,
            *[dma((nf,))] * 6,
            dma, dma,
            dma, dma((npr, cpp)),
        ],
        compiler_params=pltpu.CompilerParams(
            collective_id=0, has_side_effects=True, vmem_limit_bytes=40 * 1024 * 1024
        ),
        name="layer",
    )(*[pltpu.with_memory_space_constraint(a, pltpu.HBM) for a in (lengths, owners, hidden_in, w_query, w_key, w_value)])
    onchip = [pltpu.with_memory_space_constraint(o, pltpu.VMEM) for o in out]
    block = pl.BlockSpec
    mixed, quad, low, nq, nl = pl.pallas_call(
        functools.partial(finish, (nf, heads, npr, per)),
        out_shape=(
            jax.ShapeDtypeStruct((npr, span, heads * head_dim), BF),
            jax.ShapeDtypeStruct((npr, H, per, head_dim), F32),
            jax.ShapeDtypeStruct((npr, FD + 1, heads, head_dim), F32),
            jax.ShapeDtypeStruct((npr, H, per), F32),
            jax.ShapeDtypeStruct((npr, heads, FD + 1), F32),
        ),
        in_specs=[block(memory_space=pltpu.VMEM)] * 5,
        out_specs=[block(memory_space=pl.ANY)] * 2 + [block(memory_space=pltpu.VMEM)] * 3,
        scratch_shapes=[
            vm((npr, span, heads * head_dim), BF),
            vm((npr, H, per, head_dim), F32),
            dma((2, npr)),
        ],
        compiler_params=pltpu.CompilerParams(vmem_limit_bytes=16 * 1024 * 1024),
        name="finish",
    )(*onchip)
    return (mixed, quad[None], jnp.transpose(low, (0, 2, 1, 3))[None], nq[None], nl[None])


def solution(mesh):
    placed = (P(None, "seq", None), P(), P(), P(None, "feat"), P(), P())
    return jax.shard_map(
        body,
        mesh=mesh,
        in_specs=placed,
        out_specs=(
            P(None, "seq", "feat"),
            P("seq", None, None, "feat", None),
            P("seq", None, "feat", None, None),
            P("seq", None, None, "feat"),
            P("seq", None, "feat", None),
        ),
        check_vma=False,
    )
```

```python
import functools

import jax
import jax.numpy as jnp
from jax import lax
from jax.experimental import pallas as pl
from jax.experimental.pallas import tpu as pltpu
from jax.sharding import PartitionSpec as P

H = 16
FD = 16
NORM_FLOOR = 0.0001
LANES = 128
BF = jnp.bfloat16
F32 = jnp.float32
LIN = 128
FAR = 144
ONE = 152
LIVE_ROWS = 153

NN = (((1,), (0,)), ((), ()))
NT = (((1,), (1,)), ((), ()))
TN = (((0,), (0,)), ((), ()))


def dot(a, b, dims=NN, precision=None):
    return lax.dot_general(a, b, dims, preferred_element_type=F32, precision=precision)


def iota(shape, axis):
    return lax.broadcasted_iota(jnp.int32, shape, axis)


def features(t, rows, weights):
    diag, off, lin = weights
    tokens = t.shape[1]
    blocks = [t * t * diag if diag != 1.0 else t * t]
    scaled = t * off if off != 1.0 else t
    for o in range(1, FD // 2):
        blocks.append(scaled * pltpu.roll(t, FD - o, 0))
    blocks.append(t * lin if lin != 1.0 else t)
    blocks.append(scaled[: FD // 2] * t[FD // 2 :])
    blocks.append((iota((rows - ONE, tokens), 0) == 0).astype(F32))
    return jnp.concatenate(blocks, axis=0)


def pick_matrix(first_row, count, rows):
    r = iota((count, rows), 0) + first_row
    c = iota((count, rows), 1)
    i, j = r >> 4, r & 15
    o = (j - i) & 15
    place = jnp.where(
        o < 8, o * FD + i, jnp.where(o == 8, FAR + jnp.minimum(i, j), (FD - o) * FD + j)
    )
    return (place == c)


def kernel(cfg, len_hbm, own_hbm, x_hbm, wq_hbm, wk_hbm, wv_hbm,
           att_out, sqgot, quad_out, low_out, mine_out,
           hid, wall, qs, ks, vs, kt, phs, nd, part, mgot, bsum, up_got, up_send, dn_got, dn_send,
           fwd, pre, bwd, suf, tsend, sqsend, pick, len_ref, own_ref,
           in_sem, s0, r0, s1, r1, s2, r2, s3, r3, s4, r4, s5, r5, s8, s9, s12, r12, s7, r7):
    n, nf, npr, span, heads, rows, cpp, lag, turn, direct = cfg
    relayed = npr - direct
    me, fi = lax.axis_index("seq"), lax.axis_index("feat")
    own = heads * FD
    half = heads // 2
    last = n // 2 - 1
    zo, yi = me // 2, lax.rem(me, 2)
    mate = me + 1 - 2 * yi
    head_dim = vs.shape[2] // heads
    spot = lax.rem(fi * own, LANES)
    hw = half * head_dim
    chunks = npr * cpp
    below, above = zo > 0, zo < last

    def half_cols(c):
        return pl.ds(pl.multiple_of(c * hw, LANES), hw)

    base = pl.multiple_of((fi * own // LANES) * LANES, LANES)
    middle = wall.shape[0] // 2
    parts = (pl.ds(0, middle), pl.ds(middle, middle))

    def first_loads(i):
        r, sems = parts[i], in_sem.at[npr + i]
        mate_cols = half_cols(1 - yi)
        return [
            pltpu.make_async_copy(x_hbm.at[0, :, r], hid.at[0, :, r], sems.at[0]),
            pltpu.make_async_copy(wq_hbm.at[r, pl.ds(base, LANES)], wall.at[r, pl.ds(0, LANES)], sems.at[1]),
            pltpu.make_async_copy(wk_hbm.at[r, pl.ds(base, LANES)], wall.at[r, pl.ds(LANES, LANES)], sems.at[2]),
            pltpu.make_async_copy(wv_hbm.at[r, mate_cols], wall.at[r, pl.ds(2 * LANES, hw)], sems.at[3]),
        ]

    own_load = pltpu.make_async_copy(wv_hbm.at[:, half_cols(yi)], wall.at[:, pl.ds(2 * LANES + hw, hw)], in_sem.at[0, 0])
    small = [
        pltpu.make_async_copy(len_hbm, len_ref, in_sem.at[0, 1]),
        pltpu.make_async_copy(own_hbm, own_ref, in_sem.at[0, 2]),
    ]

    def hid_copy(p):
        return pltpu.make_async_copy(x_hbm.at[p], hid.at[p], in_sem.at[p, 3])

    for i in range(2):
        for load in first_loads(i):
            load.start()
    for load in small:
        load.start()
    own_load.start()

    barrier = pltpu.get_barrier_semaphore()

    def greet(**target):
        pl.semaphore_signal(barrier, 1, device_id=target, device_id_type=pl.DeviceIdType.MESH)

    greet(seq=mate)

    @pl.when(below)
    def _():
        greet(seq=me - 2)

    @pl.when(above)
    def _():
        greet(seq=me + 2)

    for i in range(1, nf):
        greet(feat=lax.rem(fi + i, nf))
        greet(seq=mate, feat=lax.rem(fi + i, nf))

    sqsend[...] = jnp.zeros_like(sqsend)
    pick[...] = pick_matrix(0, FD * FD, rows).astype(BF)
    send_pre, take_pre = below | (yi == 0), below | (yi == 1)
    send_suf, take_suf = above | (yi == 1), above | (yi == 0)

    @pl.when(zo == 0)
    def _():
        up_got[...] = jnp.zeros(up_got.shape, BF)

    @pl.when(zo == last)
    def _():
        dn_got[...] = jnp.zeros(dn_got.shape, BF)

    @pl.when(jnp.logical_not(take_pre))
    def _():
        pre[:, 0] = jnp.zeros((npr,) + pre.shape[2:], BF)

    @pl.when(jnp.logical_not(take_suf))
    def _():
        suf[...] = jnp.zeros(suf.shape, BF)

    def to_seq(src, dst, ssem, rsem, target):
        return pltpu.make_async_remote_copy(
            src_ref=src, dst_ref=dst, send_sem=ssem, recv_sem=rsem,
            device_id={"seq": target}, device_id_type=pl.DeviceIdType.MESH)

    def to_feat(src, dst, ssem, rsem, target):
        return pltpu.make_async_remote_copy(
            src_ref=src, dst_ref=dst, send_sem=ssem, recv_sem=rsem,
            device_id={"feat": target}, device_id_type=pl.DeviceIdType.MESH)

    def to_mates(src, dst, ssem, rsem, target):
        return pltpu.make_async_remote_copy(
            src_ref=src, dst_ref=dst, send_sem=ssem, recv_sem=rsem,
            device_id={"seq": mate, "feat": target}, device_id_type=pl.DeviceIdType.MESH)

    fpeer = lax.rem(fi + 1, nf)

    def swap_copy(p, j):
        return to_seq(part.at[p, 0, j], mgot.at[p, j], s0, r0.at[p, j], mate)

    def up_copy(p, j):
        return to_seq(up_send.at[p, j], up_got.at[p, j], s1, r1.at[p, j], me + 2 * above.astype(jnp.int32) - 2 * (1 - above.astype(jnp.int32)))

    def dn_copy(p, j):
        return to_seq(dn_send.at[p, j], dn_got.at[p, j], s2, r2.at[p, j], me - 2 * below.astype(jnp.int32) + 2 * (1 - below.astype(jnp.int32)))

    def pre_copy(p, j):
        return to_seq(fwd.at[p, j], pre.at[p, 0, j], s3, r3.at[p, j], mate)

    def suf_copy(p, j):
        return to_seq(bwd.at[p, j], suf.at[p, j], s7, r7.at[p, j], mate)

    def live_row(p):
        return ((iota((1, span), 1) + me * span) < len_ref[p]).astype(F32)

    tail = rows - ONE
    weights = (0.5 / FD, 1.0 / FD, FD ** -0.5)

    def sums_of(slot, side, v, live):
        row = iota((tail, LANES), 0)
        ones = jnp.ones((tail, span), BF)
        gap = jnp.zeros((tail, 2 * LANES - ONE - 8), F32)
        sums = []
        for h in range(half):
            phi = (features(kt[side, head_rows(slot + h)], rows, (1.0, 1.0, 1.0)) * live).astype(BF)
            summed = dot(phi, v[:, h * head_dim:(h + 1) * head_dim])
            zh = dot(ones, phi, NT)
            more = jnp.concatenate([zh[:, LANES:ONE + 8], gap], axis=1)
            end = summed[ONE:] + jnp.where(row == 1, zh[:, :LANES], 0.0) + jnp.where(row == 2, more, 0.0)
            sums.append(jnp.concatenate([summed[:ONE], end], axis=0).astype(BF))
        return jnp.concatenate(sums, axis=0).reshape(part.shape[2:])

    def head_of(slot):
        return (1 - yi if slot < half else yi) * half + slot % half

    def head_rows(slot):
        return pl.ds(pl.multiple_of(spot + head_of(slot) * FD, FD), FD)

    def project(p, first):
        cols = slice(0, 2 * LANES + hw)
        if first:
            for load in first_loads(0):
                load.wait()
            head = dot(hid[p, :, :middle], wall[:middle, cols])
            for load in first_loads(1):
                load.wait()
            for later in range(1, npr):
                hid_copy(later).start()
            head = head + dot(hid[p, :, middle:], wall[middle:, cols])
        else:
            hid_copy(p).wait()
            head = dot(hid[p], wall[:, cols])
        k = head[:, LANES:2 * LANES].astype(BF)
        qs[p] = head[:, :LANES].astype(BF)
        ks[p] = k
        slot = lax.rem(p, 2)
        kt[slot] = k.astype(F32).T
        v = head[:, 2 * LANES:].astype(BF)
        vs[p, :, :hw] = v
        mine_cols = slice(2 * LANES + hw, 2 * LANES + 2 * hw)

        def own_values():
            return jnp.concatenate(
                [dot(hid[p, r * span // 2:(r + 1) * span // 2], wall[:, mine_cols]) for r in range(2)], axis=0).astype(BF)

        if first:
            for load in small:
                load.wait()
        else:
            late(p - 1)
            mine = own_values()
        part[p, 0] = sums_of(0, slot, v, live_row(p))
        if first:
            pl.semaphore_wait(barrier, 2 * nf - 1 + below.astype(jnp.int32) + above.astype(jnp.int32))
        for j in range(cpp):
            swap_copy(p, j).start()
        if first:
            own_load.wait()
            mine = own_values()
        vs[p, :, hw:] = mine

    def late(p):
        part[p, 1] = sums_of(half, lax.rem(p, 2), vs[p, :, hw:], live_row(p))

    def pair(k):
        p, j = k // cpp, lax.rem(k, cpp)
        swap_copy(p, j).wait_recv()
        bsum[p, j] = (part[p, 1, j].astype(F32) + mgot[p, j].astype(F32)).astype(BF)

    def take_up(k):
        p, j = k // cpp, lax.rem(k, cpp)

        @pl.when(below)
        def _():
            up_copy(p, j).wait_recv()
        before = up_got[p, j].astype(F32)

        @pl.when(above)
        def _():
            up_send[p, j] = (up_got[p, j].astype(F32) + bsum[p, j].astype(F32)).astype(BF)
            up_copy(p, j).start()
        fwd[p, j] = (before + jnp.where(yi == 0, part[p, 1, j].astype(F32), 0.0)).astype(BF)

        @pl.when(below)
        def _():
            pre_copy(p, j).start()
        pre[p, 1, j] = (before + jnp.where(yi == 1, mgot[p, j].astype(F32), 0.0)).astype(BF)

    def take_down(k):
        p, j = k // cpp, lax.rem(k, cpp)

        @pl.when(above)
        def _():
            dn_copy(p, j).wait_recv()
        after = dn_got[p, j].astype(F32)

        @pl.when(below)
        def _():
            dn_send[p, j] = (dn_got[p, j].astype(F32) + bsum[p, j].astype(F32)).astype(BF)
            dn_copy(p, j).start()
        bwd[p, j] = (after + jnp.where(yi == 1, part[p, 1, j].astype(F32), 0.0)).astype(BF)

        @pl.when(above & (p < relayed))
        def _():
            suf_copy(p, j).start()

    def at(t, body, stride=1):
        @pl.when((t >= 0) & (t < chunks) & (lax.rem(t, stride) == 0))
        def _():
            body(t // stride)

    def chain(t):
        at(t, pair)
        at(t - lag * zo, take_up)
        at(t - lag * (last - zo), take_down)

    project(0, True)

    @pl.loop(1, npr)
    def _(p):
        project(p, False)

        @pl.loop(jnp.maximum(p - 2, 0) * cpp, (p - 1) * cpp)
        def _(t):
            chain(t)

    late(npr - 1)
    for p in range(npr):
        mine_out[p] = jnp.where(iota(mine_out.shape[1:], 0) == 1, len_ref[p].astype(F32), (own_ref[p] == me).astype(F32))

    def inner(p):
        causal = iota((span, span), 0) >= iota((span, span), 1)
        keep = jnp.where(causal, live_row(p), 0.0)
        ones = jnp.ones((span, head_dim), BF)
        lane = iota((1, LANES), 1) // FD
        q, k = qs[p], ks[p].astype(F32)
        kt[0] = q.astype(F32).T
        for h in range(heads):
            mask = (lane == spot // FD + head_of(h)).astype(F32)
            s = dot(q, (k * mask).astype(BF), NT)
            w = ((1.0 + s * (FD ** -0.5 + s * (0.5 / FD))) * keep).astype(BF)
            vv = jnp.concatenate([vs[p, :, h * head_dim:(h + 1) * head_dim], ones], axis=1)
            nd[p, h] = dot(w, vv)
            phs[p, h] = features(kt[0, head_rows(h)], rows, weights).astype(BF).T


    def flat(block):
        return block.reshape(half * rows, head_dim)

    def zrow_of(state):
        block = state[LIN:ONE + 8].astype(F32)
        return jnp.concatenate([block[ONE + 1 - LIN:ONE + 2 - LIN], block[ONE + 2 - LIN:ONE + 3 - LIN, :ONE + 8 - LANES]], axis=1)

    def outer(p, mates):
        live = (iota((span, 1), 0) + me * span < len_ref[p]).astype(F32)
        earlier = jnp.minimum(me * span, len_ref[p]).astype(F32)
        squares = jnp.zeros((span, head_dim), F32)
        for i in range(half):
            slot = i if mates else half + i
            head = (1 - yi if mates else yi) * half + i
            state = pre[p, 0 if mates else 1, i]
            zr = zrow_of(state)
            zr = jnp.where(iota(zr.shape, 1) == ONE, 0.0, zr)
            zb = jnp.broadcast_to(zr, (head_dim, zr.shape[1])).astype(BF)
            phit = phs[p, slot]
            num = dot(phit, state) + nd[p, slot, :, :head_dim]
            den = dot(phit[:, :zr.shape[1]], zb, NT) + nd[p, slot, :, head_dim:] + earlier
            att = num / den * live
            att_out[p, :, pl.ds(pl.multiple_of(head * head_dim, LANES), head_dim)] = att
            squares = squares + att * att
        sq = dot(jnp.ones((sqsend.shape[0], head_dim), BF), squares.astype(BF), NT)
        sqsend[...] += jnp.where(iota(sq.shape, 0) == p, sq, 0.0)

    def outer_own(p):
        outer(p, False)

    def outer_other(p):
        @pl.when(take_pre)
        def _():
            for j in range(cpp):
                pre_copy(p, j).wait_recv()
        outer(p, True)

        @pl.when(p == npr - 1)
        def _():
            sqgot[fi] = sqsend[...]
            for i in range(1, nf):
                to_feat(sqsend, sqgot.at[fi], s4.at[i], r4.at[fi], lax.rem(fi + i, nf)).start()

    per = FD * FD // nf

    def spread(p, c, totals):
        mine = [total.astype(BF) for total in totals]
        full = dot(pick[...], jnp.concatenate(mine, axis=1)).astype(BF)
        zrows = [zrow_of(m) for m in mine]
        fill = jnp.zeros((8 - half, zrows[0].shape[1]), F32)
        zq = dot(jnp.concatenate(zrows + [fill], axis=0).astype(BF), pick[...], NT)
        blank = jnp.zeros((8, head_dim - per), F32)
        for f in range(nf):
            for i in range(half):
                tsend[f, p, c, i * per:(i + 1) * per] = full[f * per:(f + 1) * per, i * head_dim:(i + 1) * head_dim]
            tsend[f, p, c, half * per:] = jnp.concatenate([zq[:, f * per:(f + 1) * per], blank], axis=1).astype(BF)
        last_one = p >= relayed

        @pl.when(jnp.logical_not(last_one))
        def _():
            for i in range(1, nf):
                target = lax.rem(fi + i, nf)
                to_feat(tsend.at[target, p, c], quad_out.at[fi, p, c], s5.at[i], r5.at[fi], target).start()
        quad_out[fi, p, c] = tsend[fi, p, c]
        for i in range(half):
            end = mine[i][LIN:].astype(F32)
            lows = end[:FD] * FD ** -0.25
            count = jnp.where(iota((1, 1), 0) == 0, len_ref[p].astype(F32), 0.0)
            zlow = jnp.concatenate([count, end[ONE + 2 - LIN:ONE + 3 - LIN, :FD] * FD ** -0.25, jnp.zeros((1, head_dim - FD - 1), F32)], axis=1)
            low_out[p, c * half + i] = jnp.concatenate(
                [end[ONE - LIN:ONE - LIN + 1], lows, zlow, jnp.zeros((6, head_dim), F32)], axis=0)


    def low_copy(p, c):
        which = pl.ds(c * half, half)
        return to_seq(low_out.at[p, which], low_out.at[p, which], s12, r12, mate)

    def spread_own(p):
        spread(p, yi, [up_got[p, j].astype(F32) + bsum[p, j].astype(F32) + dn_got[p, j].astype(F32) for j in range(cpp)])

    def spread_other(p):
        @pl.when(take_suf)
        def _():
            for j in range(cpp):
                suf_copy(p, j).wait_recv()
        spread(p, 1 - yi, [pre[p, 0, j].astype(F32) + part[p, 0, j].astype(F32) + suf[p, j].astype(F32) for j in range(cpp)])

    def held_pre(k):
        pre_copy(k // cpp, lax.rem(k, cpp)).start()

    def held_suf(k):
        @pl.when(k < relayed * cpp)
        def _():
            suf_copy(k // cpp, lax.rem(k, cpp)).start()

    early = (npr - 2) * cpp
    reach = max(lag * last, early + npr)
    far = jnp.maximum(lag * jnp.maximum(zo, last - zo), early)

    hold = early

    def step(t, _):
        chain(t)
        at(t - jnp.where(jnp.logical_not(below) & send_pre, hold, chunks + t), held_pre)
        at(t - jnp.where(jnp.logical_not(above) & send_suf, hold, chunks + t), held_suf)
        at((t - early) * 2, inner, cpp)
        base_own = jnp.where(below, reach, early + npr)
        back = t - cpp + 1
        at(back - base_own - turn, outer_other, cpp)
        at(back - far, spread_own, cpp)
        at(back - base_own, outer_own, cpp)
        mine = back - reach - turn
        at(jnp.where(mine < relayed * cpp, mine, -1), spread_other, cpp)
        return 0

    lax.fori_loop(early, chunks + reach + turn, step, 0)

    ends, starts = pl.ds(relayed, direct), pl.ds(0, relayed)
    own_side, mate_side = pl.ds(yi * half, half), pl.ds((1 - yi) * half, half)
    for i in range(1, nf):
        src = lax.rem(fi + i, nf)
        to_feat(sqsend, sqgot.at[src], s4.at[i], r4.at[src], fpeer).wait_recv()
        to_feat(tsend.at[src], quad_out.at[src], s5.at[i], r5.at[src], fpeer).wait_recv()
    for i in range(1, nf):
        to_feat(sqsend, sqgot.at[fi], s4.at[i], r4.at[fi], fpeer).wait_send()
        to_feat(tsend.at[fi, starts], quad_out.at[fi, starts], s5.at[i], r5.at[fi], fpeer).wait_send()
    to_seq(fwd, fwd, s0, s0, mate).wait_send()

    @pl.when(send_pre)
    def _():
        to_seq(fwd, fwd, s3, s3, mate).wait_send()

    @pl.when(send_suf)
    def _():
        to_seq(bwd.at[starts], bwd.at[starts], s7, s7, mate).wait_send()

    @pl.when(above)
    def _():
        to_seq(up_send, up_send, s1, s1, mate).wait_send()

    @pl.when(below)
    def _():
        to_seq(dn_send, dn_send, s2, s2, mate).wait_send()


def finish(cfg, att, sq, quad, low, mine, mixed_out, quad_out, low_out, nq_out, nl_out,
           mixed_buf, quad_buf, sem):
    nf, heads, npr, per = cfg
    span, width = att.shape[1], att.shape[2]
    half = heads // 2
    scale = (2.0 * FD) ** -0.5
    squares = sq[0]
    for f in range(1, nf):
        squares = squares + sq[f]
    inv = lax.rsqrt(squares * (1.0 / (nf * width)) + NORM_FLOOR)
    writes = []
    for p in range(npr):
        mask = mine[p, :1] * scale
        for f in range(nf):
            for c in range(2):
                block = quad[f, p, c].astype(F32) * mask
                for i in range(half):
                    quad_buf[p, f * heads + c * half + i] = block[i * per:(i + 1) * per]
                nq_out[p, f * heads + c * half:f * heads + (c + 1) * half] = block[half * per:half * per + half, :per]
        writes.append(pltpu.make_async_copy(quad_buf.at[p], quad_out.at[p], sem.at[0, p]))
        writes[-1].start()
        col = jnp.broadcast_to(inv[p:p + 1], (LANES, span)).T
        for c in range(width // LANES):
            mixed_buf[p, :, c * LANES:(c + 1) * LANES] = (att[p, :, c * LANES:(c + 1) * LANES] * col).astype(BF)
        writes.append(pltpu.make_async_copy(mixed_buf.at[p], mixed_out.at[p], sem.at[1, p]))
        writes[-1].start()
    for p in range(npr):
        for h in range(heads):
            full = low[p, h] * mine[p, :1]
            low_out[p, :, h, :] = full[:FD + 1]
            nl_out[p, h:h + 1] = full[FD + 1:FD + 2, :FD + 1]
    for write in writes:
        write.wait()


def body(hidden_in, w_query, w_key, w_value, lengths, owners):
    npr, span, width = hidden_in.shape
    n, nf = lax.axis_size("seq"), lax.axis_size("feat")
    heads = H // nf
    head_dim = width // H
    rows = -(-LIVE_ROWS // 16) * 16
    half_rows = heads // 2 * rows
    cpp, lag, turn = heads // 2, 4, 3
    cfg = (n, nf, npr, span, heads, rows, cpp, lag, turn, 0)
    per = FD * FD // nf
    chunk = (cpp, half_rows // cpp, head_dim)
    dma = pltpu.SemaphoreType.DMA
    vm = pltpu.VMEM
    out = pl.pallas_call(
        functools.partial(kernel, cfg),
        out_shape=(
            vm((npr, span, heads * head_dim), F32),
            vm((nf, 8, span), F32),
            vm((nf, npr, 2, heads // 2 * per + 8, head_dim), BF),
            vm((npr, heads, 24, head_dim), F32),
            vm((npr, 8, LANES), F32),
        ),
        in_specs=[pl.BlockSpec(memory_space=pltpu.HBM)] * 6,
        out_specs=[pl.BlockSpec(memory_space=pltpu.VMEM)] * 5,
        scratch_shapes=[
            vm((npr, span, width), BF),
            vm((width, 2 * LANES + heads * head_dim), BF),
            vm((npr, span, LANES), BF),
            vm((npr, span, LANES), BF),
            vm((npr, span, heads * head_dim), BF),
            vm((2, LANES, span), F32),
            vm((npr, heads, span, rows), BF),
            vm((npr, heads, span, 2 * head_dim), F32),
            vm((npr, 2) + chunk, BF),
            *[vm((npr,) + chunk, BF)] * 7,
            vm((npr, 2) + chunk, BF),
            *[vm((npr,) + chunk, BF)] * 2,
            vm((nf, npr, 2, heads // 2 * per + 8, head_dim), BF),
            vm((8, span), F32),
            vm((FD * FD, rows), BF),
            pltpu.SMEM((npr,), jnp.int32),
            pltpu.SMEM((npr,), jnp.int32),
            dma((npr + 2, 4)),
            *[dma, dma((npr, cpp))] * 4,
            *[dma((nf,))] * 6,
            dma, dma,
            dma, dma((npr, cpp)),
        ],
        compiler_params=pltpu.CompilerParams(
            collective_id=0, has_side_effects=True, vmem_limit_bytes=40 * 1024 * 1024
        ),
        name="layer",
    )(*[pltpu.with_memory_space_constraint(a, pltpu.HBM) for a in (lengths, owners, hidden_in, w_query, w_key, w_value)])
    onchip = [pltpu.with_memory_space_constraint(o, pltpu.VMEM) for o in out]
    block = pl.BlockSpec
    mixed, quad, low, nq, nl = pl.pallas_call(
        functools.partial(finish, (nf, heads, npr, per)),
        out_shape=(
            jax.ShapeDtypeStruct((npr, span, heads * head_dim), BF),
            jax.ShapeDtypeStruct((npr, H, per, head_dim), F32),
            jax.ShapeDtypeStruct((npr, FD + 1, heads, head_dim), F32),
            jax.ShapeDtypeStruct((npr, H, per), F32),
            jax.ShapeDtypeStruct((npr, heads, FD + 1), F32),
        ),
        in_specs=[block(memory_space=pltpu.VMEM)] * 5,
        out_specs=[block(memory_space=pl.ANY)] * 2 + [block(memory_space=pltpu.VMEM)] * 3,
        scratch_shapes=[
            vm((npr, span, heads * head_dim), BF),
            vm((npr, H, per, head_dim), F32),
            dma((2, npr)),
        ],
        compiler_params=pltpu.CompilerParams(vmem_limit_bytes=16 * 1024 * 1024),
        name="finish",
    )(*onchip)
    return (mixed, quad[None], jnp.transpose(low, (0, 2, 1, 3))[None], nq[None], nl[None])


def solution(mesh):
    placed = (P(None, "seq", None), P(), P(), P(None, "feat"), P(), P())
    return jax.shard_map(
        body,
        mesh=mesh,
        in_specs=placed,
        out_specs=(
            P(None, "seq", "feat"),
            P("seq", None, None, "feat", None),
            P("seq", None, "feat", None, None),
            P("seq", None, None, "feat"),
            P("seq", None, "feat", None),
        ),
        check_vma=False,
    )
```
